32 devices in a mesh: chan: 8 (over z, core), band: 4 (over y, x).
Axes of the slice: x: 2, y: 2, z: 4, core: 2. Of those that a mesh axis runs over, the one named last changes fastest.
Arguments:
- residual: float32 [64, 96, 16384], P('chan', 'band'), may hold values from -60 to 60
- weight_index: int32 [64], P('chan'), may hold values from 0 to 15
- weight_table: float32 [16], replicated, may hold values from 0.2 to 5
- gridded: float32 [2, 8, 128, 16384], P(None, 'chan', 'band'), may hold values from -6 to 6
Outputs:
- components: float32 [3, 96, 16384], P(None, 'band', 'chan')
- spectrum: float32 [2, 8, 16384, 128], P(None, 'chan', 'band')
The draws below stay inside these ranges and needn't reach their ends.
All inputs are finite; a program needn't handle non-finite values.
Results may differ from the reference program's by a relative error of at most 0.0002.
Values sent between devices are 32-bit elements; how exact they have to be, the bound alone decides.
A program may use at most 128 MiB of HBM per device.

```python
import math
import jax
import jax.numpy as jnp
from jax import lax

IMG = 16384
GRID = 16384
NW = 16
CHANNELS = 64
IMG_ROWS = 96
ROWS = 128
GROUPS = 8


def draw_residual(key, part):
    key_sky, key_noise = jax.random.split(jax.random.fold_in(key, 11), 2)
    position = jnp.arange(CHANNELS, dtype=jnp.float32)
    offset = (2.0 * position + 1.0) / CHANNELS - 1.0
    amplitude = jnp.array([1.0, 0.7, 0.5], dtype=jnp.float32)
    sky = jax.random.normal(key_sky, (3, IMG_ROWS, IMG), jnp.float32) * amplitude[:, None, None]
    noise = 3.0 * jax.random.normal(key_noise, (CHANNELS, IMG_ROWS, IMG), jnp.float32)
    values = sky[0][None] + offset[:, None, None] * sky[1][None] + (offset * offset)[:, None, None] * sky[2][None] + noise
    return jnp.clip(values, -60.0, 60.0)


def touch_ends(entries, rng, smallest, high):
    longest = entries.shape.index(max(entries.shape))
    spots = []
    for shift in (0, 1):
        where = [jax.random.randint(jax.random.fold_in(rng, axis), (), 0, length) for axis, length in enumerate(entries.shape)]
        where[longest] = (where[longest] + shift) % entries.shape[longest]
        spots.append(tuple(where))
    return entries.at[spots[0]].set(smallest).at[spots[1]].set(high)


def levels(stream_key, shape, cuts, low, top_value):
    def one(dim, blocks):
        heights = jax.random.uniform(jax.random.fold_in(jax.random.fold_in(stream_key, 6), dim), (blocks,), jnp.float32, low / len(cuts), top_value / len(cuts))
        return jnp.repeat(jnp.exp(heights), shape[dim] // blocks).reshape((-1,) + (1,) * (len(shape) - dim - 1))

    gain = one(*cuts[0])
    for cut in cuts[1:]:
        gain = gain * one(*cut)
    return gain


def normal_values(stream_key, shape, width, most, cuts=(), kind=jnp.bfloat16):
    values = width * jax.random.normal(stream_key, shape, jnp.float32)
    if cuts:
        values = values * levels(stream_key, shape, cuts, -0.22, 0.18)
    return jnp.clip(values, -most, most).astype(kind)


def setup_inputs(seed: int = 0) -> dict:
    key_of = jax.random.split(jax.random.key(seed), 5)
    return {
        "residual": draw_residual(jax.random.fold_in(key_of[4], 71), 0),
        "weight_index": touch_ends(jax.random.randint(key_of[1], (CHANNELS,), 0, NW), jax.random.fold_in(key_of[1], 1), 0, NW - 1).astype(jnp.int32),
        "weight_table": jnp.clip(jnp.exp(jax.random.uniform(key_of[2], (NW,), jnp.float32, math.log(0.2), math.log(5.0))), 0.2, 5.0),
        "gridded": normal_values(key_of[3], (2, GROUPS, ROWS, GRID), 1.0, 6.0, ((1, 8), (2, 4)), jnp.float32),
    }


def channel_terms(weight_index, weight_table, first, total):
    count = weight_index.shape[0]
    position = (first + jnp.arange(count, dtype=jnp.int32)).astype(jnp.float32)
    offset = (2.0 * position + 1.0) / total - 1.0
    slots = jnp.arange(weight_table.shape[0], dtype=jnp.int32)
    onehot = (weight_index[:, None] == slots[None, :]).astype(jnp.float32)
    weights = jnp.dot(onehot, weight_table, precision=lax.Precision.HIGHEST)
    return (weights, offset)

def solve_terms(moment, taylor):
    sum_zero, sum_one, sum_two, sum_three, sum_four = (moment[0], moment[1], moment[2], moment[3], moment[4])
    entry_aa = sum_two * sum_four - sum_three * sum_three
    entry_ab = sum_two * sum_three - sum_one * sum_four
    entry_ac = sum_one * sum_three - sum_two * sum_two
    entry_bb = sum_zero * sum_four - sum_two * sum_two
    entry_bc = sum_one * sum_two - sum_zero * sum_three
    entry_cc = sum_zero * sum_two - sum_one * sum_one
    determ = sum_zero * entry_aa + sum_one * entry_ab + sum_two * entry_ac
    inverse = jnp.stack([jnp.stack([entry_aa, entry_ab, entry_ac]), jnp.stack([entry_ab, entry_bb, entry_bc]), jnp.stack([entry_ac, entry_bc, entry_cc])]) / determ
    return jnp.einsum('ts,sij->tij', inverse, taylor, precision=lax.Precision.HIGHEST)

def reference(residual, weight_index, weight_table, gridded):
    weights, offset = channel_terms(weight_index, weight_table, 0, CHANNELS)
    coeffs = jnp.stack([weights, weights * offset, weights * offset * offset])
    flat = residual.reshape(residual.shape[0], -1)
    taylor = jnp.dot(coeffs, flat, precision=lax.Precision.HIGHEST).reshape(3, residual.shape[1], residual.shape[2])
    moment = jnp.stack([jnp.sum(weights * offset ** power) for power in range(5)])
    components = solve_terms(moment, taylor)
    field = gridded[0] + 1j * gridded[1]
    transformed = jnp.fft.fft(field, axis=-1) / jnp.sqrt(jnp.float32(GRID))
    stacked = jnp.stack([jnp.real(transformed), jnp.imag(transformed)]).astype(jnp.float32)
    spectrum = jnp.swapaxes(stacked, 2, 3)
    return (components, spectrum)
```

```python
import functools
import math

import jax
import jax.numpy as jnp
import numpy as np
from jax import lax
from jax.experimental import pallas as pl
from jax.experimental.pallas import tpu as pltpu
from jax.sharding import PartitionSpec as P

MESH = pl.DeviceIdType.MESH
LANES = 128
SUB = 8
AHEAD = 2


def block_form(table):
    real = np.block([[table.real, -table.imag], [table.imag, table.real]]).astype(np.float32)
    high = real.astype(jnp.bfloat16)
    low = (real - high.astype(np.float32)).astype(jnp.bfloat16)
    return np.concatenate([high, low, high], axis=1)


def dft(size):
    grid = np.outer(np.arange(size), np.arange(size)) % size
    return np.exp(-2j * np.pi * grid / size)


def tables(length):
    outer = length // LANES
    turn = np.exp(-2j * np.pi * np.outer(np.arange(outer), np.arange(LANES)) / length)
    turn = turn / math.sqrt(length)
    bases = [block_form(dft(outer))]
    if outer != LANES:
        bases.append(block_form(dft(LANES)))
    return (np.stack([turn.real, turn.imag]).astype(np.float32), *bases)


def inverse_rows(moment):
    s0, s1, s2, s3, s4 = (moment[j : j + 1, :] for j in range(5))
    aa = s2 * s4 - s3 * s3
    ab = s2 * s3 - s1 * s4
    ac = s1 * s3 - s2 * s2
    bb = s0 * s4 - s2 * s2
    bc = s1 * s2 - s0 * s3
    cc = s0 * s2 - s1 * s1
    determ = s0 * aa + s1 * ab + s2 * ac
    return [entry / determ for entry in (aa, ab, ac, bb, bc, cc)]


def exchange_kernel(nc, nb, bases, idx_ref, tab_ref, *rest):
    steps = int(math.log2(nc))
    tables_hbm, (res_hbm, grid_hbm) = rest[: bases + 1], rest[bases + 1 : bases + 3]
    spec_ref, comp_ref = rest[bases + 3 : bases + 5]
    rest = rest[bases + 5 :]
    tables_v, rest = rest[: bases + 1], rest[bases + 1 :]
    (grid_v, out_v, recv_v, res_v, part_v, mom_v, mom_land) = rest[:7]
    lands = rest[7 : 7 + steps]
    (tab_sem, grid_sem, res_sem, es_sem, er_sem, ls_sem, lr_sem, rs_sem, rr_sem, ms_sem, mr_sem) = rest[7 + steps :]
    turn_v, first_v, second_v = tables_v[0], tables_v[1], tables_v[-1]
    chan = lax.axis_index("chan")
    band = lax.axis_index("band")
    tiles, outer8 = grid_v.shape[1], grid_v.shape[2]
    outer = outer8 // SUB
    kept = LANES // nb
    parts = res_v.shape[0]
    count = res_v.shape[1]
    wide = part_v.shape[3]
    chunks = part_v.shape[0]
    cuts = chunks // parts
    early = tiles // 2
    late = tiles - early
    pieces = head_pieces(tiles)
    slices = ls_sem.shape[0]
    span = kept // slices

    def table_copy(j):
        return pltpu.make_async_copy(tables_hbm[j], tables_v[j], tab_sem.at[j])

    def grid_copy(t):
        return pltpu.make_async_copy(grid_hbm.at[:, t], grid_v.at[:, t], grid_sem.at[t])

    def res_copy(c):
        return pltpu.make_async_copy(
            res_hbm.at[:, pl.ds(c * SUB, SUB), :], res_v.at[c], res_sem.at[c]
        )

    bits = [(chan // (1 << s)) % 2 for s in range(steps)]
    partners = [chan + (1 - 2 * bits[s]) * (1 << s) for s in range(steps)]
    starts = [0]
    for s in range(steps):
        starts.append(starts[s] + bits[s] * (nc >> (s + 1)))

    barrier = pltpu.get_barrier_semaphore()
    for d in range(1, nb):
        peer = lax.rem(band + d, nb)
        pl.semaphore_signal(barrier, inc=1, device_id=(chan, peer), device_id_type=MESH)
    for s in range(steps):
        pl.semaphore_signal(barrier, inc=1, device_id=(partners[s], band), device_id_type=MESH)

    for j in range(bases, -1, -1):
        table_copy(j).start()
    for i in range(max(tiles, parts)):
        if i < tiles:
            grid_copy(i).start()
        if i < parts:
            res_copy(i).start()

    total = count * nc
    coeffs = []
    moments = [jnp.float32(0.0)] * 5
    for c in range(count):
        weight = tab_ref[idx_ref[c]]
        position = (chan * count + c).astype(jnp.float32)
        offset = (2.0 * position + 1.0) * (1.0 / total) - 1.0
        power = weight
        trio = []
        for j in range(5):
            if j < 3:
                trio.append(power)
            moments[j] = moments[j] + power
            power = power * offset
        coeffs.append(trio)
    line = lax.broadcasted_iota(jnp.int32, (SUB, LANES), 0)
    tile = jnp.zeros((SUB, LANES), jnp.float32)
    for j in range(5):
        tile = jnp.where(line == j, moments[j], tile)
    mom_v[0] = tile

    def transform(t, begin, stop):
        def pair(i, carry):
            cols = []
            for k in range(2):
                r = i * 2 + k
                cols.append(
                    jnp.concatenate(
                        [grid_v[p, t, pl.ds(r, outer, stride=SUB), :] for p in range(2)], axis=0
                    )
                )
            x = jnp.concatenate(cols, axis=1)
            high = x.astype(jnp.bfloat16)
            low = (x - high.astype(jnp.float32)).astype(jnp.bfloat16)
            mid = jnp.dot(
                first_v[...],
                jnp.concatenate([high, high, low], axis=0),
                preferred_element_type=jnp.float32,
            )
            turn_re, turn_im = turn_v[0], turn_v[1]
            turned = []
            for k in range(2):
                re = mid[:outer, k * LANES : (k + 1) * LANES]
                im = mid[outer:, k * LANES : (k + 1) * LANES]
                turned.append(
                    jnp.concatenate(
                        [re * turn_re - im * turn_im, re * turn_im + im * turn_re], axis=1
                    )
                )
            y = jnp.concatenate(turned, axis=0)
            high = y.astype(jnp.bfloat16)
            low = (y - high.astype(jnp.float32)).astype(jnp.bfloat16)
            out = lax.dot_general(
                second_v[...],
                jnp.concatenate([high, high, low], axis=1),
                (((1,), (1,)), ((), ())),
                preferred_element_type=jnp.float32,
            )
            flat = out_v.reshape(tiles, LANES * 2 * SUB, outer)
            for k in range(2):
                for p in range(2):
                    flat[t, pl.ds(p * SUB + i * 2 + k, LANES, stride=2 * SUB), :] = out[
                        p * LANES : (p + 1) * LANES, k * outer : (k + 1) * outer
                    ]
            return carry

        lax.fori_loop(begin // 2, stop // 2, pair, 0)

    def piece_send(j, d):
        t, begin, size = pieces[j]
        peer = lax.rem(band + d, nb)
        return pltpu.make_async_remote_copy(
            src_ref=out_v.at[t, pl.ds(peer * kept * 2, kept * 2), pl.ds(begin, size), :],
            dst_ref=recv_v.at[band * tiles + t, :, pl.ds(begin, size), :],
            send_sem=es_sem.at[j, d - 1],
            recv_sem=er_sem.at[j, d - 1],
            device_id=(chan, peer),
            device_id_type=MESH,
        )

    def slice_send(q, d):
        peer = lax.rem(band + d, nb)
        return pltpu.make_async_remote_copy(
            src_ref=out_v.at[pl.ds(early, late), pl.ds((peer * kept + q * span) * 2, span * 2)],
            dst_ref=recv_v.at[pl.ds(band * tiles + early, late), pl.ds(q * span * 2, span * 2)],
            send_sem=ls_sem.at[q, d - 1],
            recv_sem=lr_sem.at[q, d - 1],
            device_id=(chan, peer),
            device_id_type=MESH,
        )

    def keep(t):
        recv_v[band * tiles + t] = out_v[t, pl.ds(band * kept * 2, kept * 2)]

    def flip(q):
        def one(k, carry):
            for p in range(2):
                block = recv_v[:, q * span * 2 + k * 2 + p]
                spec_ref[p, 0, pl.ds(pl.multiple_of((q * span + k) * outer, LANES), outer), :] = block.reshape(
                    nb * tiles * SUB, outer
                ).T
            return carry

        lax.fori_loop(0, span, one, 0, unroll=2 if span % 2 == 0 else 1)

    def weigh(c):
        step = 512 if wide % 512 == 0 else LANES

        def one(j, carry):
            spot = 0
            for s in range(steps):
                spot = spot + ((j // (1 << s)) % 2) * (1 << (steps - 1 - s))
            for q in range(wide // step):
                col = pl.multiple_of((j * cuts + c % cuts) * wide + q * step, LANES)
                sums = [None] * 3
                for ch in range(count):
                    x = res_v[c // cuts, ch, :, pl.ds(col, step)]
                    for t in range(3):
                        term = coeffs[ch][t] * x
                        sums[t] = term if ch == 0 else sums[t] + term
                for t in range(3):
                    part_v[c, spot, pl.ds(t * SUB, SUB), pl.ds(q * step, step)] = sums[t]
            return carry

        lax.fori_loop(0, nc, one, 0)

    def half_send(c, s):
        size = nc >> (s + 1)
        begin = starts[s] + (1 - bits[s]) * size
        return pltpu.make_async_remote_copy(
            src_ref=part_v.at[c, pl.ds(begin, size)],
            dst_ref=lands[s].at[c],
            send_sem=rs_sem.at[c, s],
            recv_sem=rr_sem.at[c, s],
            device_id=(partners[s], band),
            device_id_type=MESH,
        )

    def mom_send(s):
        return pltpu.make_async_remote_copy(
            src_ref=mom_v.at[s],
            dst_ref=mom_land.at[s],
            send_sem=ms_sem.at[s],
            recv_sem=mr_sem.at[s],
            device_id=(partners[s], band),
            device_id_type=MESH,
        )

    solved = []

    def mom_add(s):
        mom_send(s).wait_recv()
        moment = mom_v[s] + mom_land[s]
        if s < steps - 1:
            mom_v[s + 1] = moment
            mom_send(s + 1).start()
            return
        for entry in inverse_rows(moment):
            solved.append(jnp.broadcast_to(entry, (SUB, LANES)))

    def half_add(c, s, send=True):
        half_send(c, s).wait_recv()
        size = nc >> (s + 1)
        if s == steps - 1:
            aa, ab, ac, bb, bc, cc = solved
            table = ((aa, ab, ac), (ab, bb, bc), (ac, bc, cc))
            for q in range(wide // LANES):
                at = pl.ds(q * LANES, LANES)
                tay = [
                    part_v[c, starts[s + 1], pl.ds(t * SUB, SUB), at] + lands[s][c, 0, pl.ds(t * SUB, SUB), at]
                    for t in range(3)
                ]
                for t, row in enumerate(table):
                    comp_ref[t, pl.ds(c // cuts * SUB, SUB), pl.ds(c % cuts * wide + q * LANES, LANES)] = (
                        row[0] * tay[0] + row[1] * tay[1] + row[2] * tay[2]
                    )
            return
        half = size // 2
        for mine in (1 - bits[s + 1], bits[s + 1]):
            for q in range(half):
                at = mine * half + q
                part_v[c, starts[s + 1] + at] = part_v[c, starts[s + 1] + at] + lands[s][c, at]
            if send and mine is not bits[s + 1]:
                half_send(c, s + 1).start()

    ahead = min(AHEAD, chunks)
    moved = 0

    def advance():
        nonlocal moved
        half_add(moved, 1)
        if moved + ahead < chunks:
            half_send(moved + ahead, 1).start()
        moved += 1

    weighed = added = 0

    def spread():
        nonlocal weighed
        c = weighed
        if c < chunks:
            if c % cuts == 0:
                res_copy(c // cuts).wait()
            weigh(c)
            half_send(c, 0).start()
        weighed += 1

    def gather():
        nonlocal added
        if added < min(weighed, chunks):
            half_add(added, 0, send=added < ahead)
            added += 1

    def piece_go(j):
        t, begin, size = pieces[j]
        transform(t, begin, begin + size)
        if j == 0:
            pl.semaphore_wait(barrier, nb - 1 + steps)
        for d in range(1, nb):
            piece_send(j, d).start()

    for j in range(bases, -1, -1):
        table_copy(j).wait()
    grid_copy(0).wait()
    for j, (t, begin, size) in enumerate(pieces):
        if begin == 0 and t > 0:
            grid_copy(t).wait()
        piece_go(j)
        if j == 0:
            mom_send(0).start()
        spread()
        if j > 0:
            gather()
            spread()
        if begin + size == SUB:
            keep(t)
            gather()
    for t in range(early, tiles):
        grid_copy(t).wait()
        transform(t, 0, SUB)
        keep(t)
        spread()
        gather()
    for q in range(slices):
        for d in range(1, nb):
            slice_send(q, d).start()
    while weighed < chunks:
        spread()
    while added < chunks:
        gather()
    for s in range(steps):
        mom_add(s)

    def open_pieces():
        for j in range(len(pieces)):
            for d in range(1, nb):
                piece_send(j, d).wait_recv()

    def flip_go(q):
        for d in range(1, nb):
            slice_send(q, d).wait_recv()
        flip(q)

    when = [(z_time(c, chunks), 0, advance, ()) for c in range(chunks)]
    for s in range(2, steps):
        for c in range(chunks):
            when.append((z_time(c + 1.5 + 2 * (s - 2), chunks) if c < chunks - 1 else 1.0 + s, s, half_add, (c, s)))
    when.append((0.5, 9, open_pieces, ()))
    for q in range(slices):
        when.append((0.5 + 0.5 * (q + 1) / slices, 10, flip_go, (q,)))
    when.sort(key=lambda job: job[:2])
    flips = [job for job in when if job[2] is flip_go]
    when.remove(flips[-1])
    when.append(flips[-1])
    for _, _, work, args in when:
        work(*args)

    for s in range(steps):
        mom_send(s).wait_send()
    for c in range(chunks):
        for s in range(steps):
            half_send(c, s).wait_send()
    for d in range(1, nb):
        for j in range(len(pieces)):
            piece_send(j, d).wait_send()
        for q in range(slices):
            slice_send(q, d).wait_send()


def z_time(c, chunks):
    return 0.25 + 0.6 * c / chunks


def head_pieces(tiles):
    early = tiles // 2
    half = SUB // 2
    return [(0, 0, half), (0, half, half)][: 2 * early] + [(t, 0, SUB) for t in range(1, early)]


def place_kernel(spec_ref, comp_ref, spec_hbm, comp_hbm, sem):
    cuts = sem.shape[0] // 2
    rows = spec_ref.shape[2] // cuts
    copies = [pltpu.make_async_copy(comp_ref, comp_hbm, sem.at[2 * cuts])]
    for p in range(2):
        for k in range(cuts):
            at = (p, 0, pl.ds(k * rows, rows))
            copies.append(pltpu.make_async_copy(spec_ref.at[at], spec_hbm.at[at], sem.at[p * cuts + k]))
    for copy in copies:
        copy.start()
    for copy in copies:
        copy.wait()


def local(nc, nb, residual, weight_index, weight_table, gridded):
    count, row_count, columns = residual.shape
    _, groups, rows, length = gridded.shape
    outer = length // LANES
    tiles, parts = rows // SUB, row_count // SUB
    wide = columns // nc
    halves = 2
    kept = LANES // nb
    slices = min(8, kept)
    steps = int(math.log2(nc))
    view = gridded.reshape(2, tiles, SUB, outer, LANES)
    view = jnp.transpose(view, (0, 1, 3, 2, 4)).reshape(2, tiles, outer * SUB, LANES)
    vmem = pl.BlockSpec(memory_space=pltpu.VMEM)
    smem = pl.BlockSpec(memory_space=pltpu.SMEM)
    hbm = pl.BlockSpec(memory_space=pl.ANY)
    dma = pltpu.SemaphoreType.DMA
    consts = [jnp.asarray(table) for table in tables(length)]
    bases = len(consts) - 1
    pieces = len(head_pieces(tiles))
    shape_spec = (2, 1, kept * outer, nb * rows)
    shape_comp = (3, row_count, wide)
    held = pl.pallas_call(
        functools.partial(exchange_kernel, nc, nb, bases),
        out_shape=(pltpu.VMEM(shape_spec, jnp.float32), pltpu.VMEM(shape_comp, jnp.float32)),
        in_specs=[smem, smem] + [hbm] * (bases + 3),
        out_specs=(vmem, vmem),
        scratch_shapes=[
            *[pltpu.VMEM(c.shape, c.dtype) for c in consts],
            pltpu.VMEM((2, tiles, outer * SUB, LANES), jnp.float32),
            pltpu.VMEM((tiles, LANES * 2, SUB, outer), jnp.float32),
            pltpu.VMEM((nb * tiles, kept * 2, SUB, outer), jnp.float32),
            pltpu.VMEM((parts, count, SUB, columns), jnp.float32),
            pltpu.VMEM((parts * halves, nc, 3 * SUB, wide // halves), jnp.float32),
            pltpu.VMEM((steps, SUB, LANES), jnp.float32),
            pltpu.VMEM((steps, SUB, LANES), jnp.float32),
            *[
                pltpu.VMEM((parts * halves, nc >> (s + 1), 3 * SUB, wide // halves), jnp.float32)
                for s in range(steps)
            ],
            dma((bases + 1,)),
            dma((tiles,)),
            dma((parts,)),
            dma((pieces, nb - 1)),
            dma((pieces, nb - 1)),
            dma((slices, nb - 1)),
            dma((slices, nb - 1)),
            dma((parts * halves, steps)),
            dma((parts * halves, steps)),
            dma((steps,)),
            dma((steps,)),
        ],
        compiler_params=pltpu.CompilerParams(
            collective_id=0, has_side_effects=True, vmem_limit_bytes=62_200_000
        ),
        name="exchange",
    )(weight_index, weight_table, *consts, residual, view)
    cuts = 4
    spectrum, components = pl.pallas_call(
        place_kernel,
        out_shape=(
            jax.ShapeDtypeStruct(shape_spec, jnp.float32),
            jax.ShapeDtypeStruct(shape_comp, jnp.float32),
        ),
        in_specs=[vmem, vmem],
        out_specs=(hbm, hbm),
        scratch_shapes=[dma((2 * cuts + 1,))],
        compiler_params=pltpu.CompilerParams(vmem_limit_bytes=16 * 1024 * 1024),
        name="place",
    )(*held)
    return (components, spectrum)


def solution(mesh):
    nc, nb = mesh.shape["chan"], mesh.shape["band"]
    in_specs = (P("chan", "band", None), P("chan"), P(), P(None, "chan", "band", None))
    out_specs = (P(None, "band", "chan"), P(None, "chan", "band", None))
    return jax.shard_map(
        functools.partial(local, nc, nb),
        mesh=mesh,
        in_specs=in_specs,
        out_specs=out_specs,
        check_vma=False,
    )
```

```python
import functools
import math

import jax
import jax.numpy as jnp
import numpy as np
from jax import lax
from jax.experimental import pallas as pl
from jax.experimental.pallas import tpu as pltpu
from jax.sharding import PartitionSpec as P

MESH = pl.DeviceIdType.MESH
LANES = 128
SUB = 8
AHEAD = 3


def block_form(table):
    real = np.block([[table.real, -table.imag], [table.imag, table.real]]).astype(np.float32)
    high = real.astype(jnp.bfloat16)
    low = (real - high.astype(np.float32)).astype(jnp.bfloat16)
    return np.concatenate([high, low, high], axis=1)


def dft(size):
    grid = np.outer(np.arange(size), np.arange(size)) % size
    return np.exp(-2j * np.pi * grid / size)


def tables(length):
    outer = length // LANES
    turn = np.exp(-2j * np.pi * np.outer(np.arange(outer), np.arange(LANES)) / length)
    turn = turn / math.sqrt(length)
    bases = [block_form(dft(outer))]
    if outer != LANES:
        bases.append(block_form(dft(LANES)))
    return (np.stack([turn.real, turn.imag]).astype(np.float32), *bases)


def inverse_rows(moment):
    s0, s1, s2, s3, s4 = (moment[j : j + 1, :] for j in range(5))
    aa = s2 * s4 - s3 * s3
    ab = s2 * s3 - s1 * s4
    ac = s1 * s3 - s2 * s2
    bb = s0 * s4 - s2 * s2
    bc = s1 * s2 - s0 * s3
    cc = s0 * s2 - s1 * s1
    determ = s0 * aa + s1 * ab + s2 * ac
    return [entry / determ for entry in (aa, ab, ac, bb, bc, cc)]


def exchange_kernel(nc, nb, bases, idx_hbm, tab_hbm, *rest):
    steps = int(math.log2(nc))
    tables_hbm, (res_hbm, grid_hbm) = rest[: bases + 1], rest[bases + 1 : bases + 3]
    spec_ref, comp_ref = rest[bases + 3 : bases + 5]
    rest = rest[bases + 5 :]
    tables_v, rest = rest[: bases + 1], rest[bases + 1 :]
    (idx_ref, tab_ref, grid_v, out_v, recv_v, res_v, part_v, mom_v, mom_land) = rest[:9]
    lands = rest[9 : 9 + steps]
    (idx_sem, tab_sem, grid_sem, res_sem, es_sem, er_sem, ls_sem, lr_sem, rs_sem, rr_sem, ms_sem, mr_sem) = rest[9 + steps :]
    turn_v, first_v, second_v = tables_v[0], tables_v[1], tables_v[-1]
    chan = lax.axis_index("chan")
    band = lax.axis_index("band")
    tiles, outer8 = grid_v.shape[1], grid_v.shape[2]
    outer = outer8 // SUB
    kept = LANES // nb
    parts = res_v.shape[0]
    count = res_v.shape[1]
    wide = part_v.shape[3]
    chunks = part_v.shape[0]
    cuts = chunks // parts
    early = tiles // 2
    late = tiles - early
    pieces = head_pieces(tiles)
    slices = ls_sem.shape[0]
    span = kept // slices

    def table_copy(j):
        return pltpu.make_async_copy(tables_hbm[j], tables_v[j], tab_sem.at[j])

    def grid_copy(t):
        return pltpu.make_async_copy(grid_hbm.at[:, t], grid_v.at[:, t], grid_sem.at[t])

    def res_copy(c):
        return pltpu.make_async_copy(
            res_hbm.at[:, pl.ds(c * SUB, SUB), :], res_v.at[c], res_sem.at[c]
        )

    bits = [(chan // (1 << s)) % 2 for s in range(steps)]
    partners = [chan + (1 - 2 * bits[s]) * (1 << s) for s in range(steps)]
    starts = [0]
    for s in range(steps):
        starts.append(starts[s] + bits[s] * (nc >> (s + 1)))

    small = [
        pltpu.make_async_copy(idx_hbm, idx_ref, idx_sem.at[0]),
        pltpu.make_async_copy(tab_hbm, tab_ref, idx_sem.at[1]),
    ]
    for j in range(bases, -1, -1):
        table_copy(j).start()
    grid_copy(0).start()
    for copy in small:
        copy.start()

    barrier = pltpu.get_barrier_semaphore()
    for d in range(1, nb):
        peer = lax.rem(band + d, nb)
        pl.semaphore_signal(barrier, inc=1, device_id=(chan, peer), device_id_type=MESH)
    for s in range(steps):
        pl.semaphore_signal(barrier, inc=1, device_id=(partners[s], band), device_id_type=MESH)

    for copy in small:
        copy.wait()
    total = count * nc
    coeffs = []
    moments = [jnp.float32(0.0)] * 5
    for c in range(count):
        weight = tab_ref[idx_ref[c]]
        position = (chan * count + c).astype(jnp.float32)
        offset = (2.0 * position + 1.0) * (1.0 / total) - 1.0
        power = weight
        trio = []
        for j in range(5):
            if j < 3:
                trio.append(power)
            moments[j] = moments[j] + power
            power = power * offset
        coeffs.append(trio)
    line = lax.broadcasted_iota(jnp.int32, (SUB, LANES), 0)
    tile = jnp.zeros((SUB, LANES), jnp.float32)
    for j in range(5):
        tile = jnp.where(line == j, moments[j], tile)
    mom_v[0] = tile

    def transform(t, begin, stop):
        def pair(i, carry):
            cols = []
            for k in range(2):
                r = i * 2 + k
                cols.append(
                    jnp.concatenate(
                        [grid_v[p, t, pl.ds(r, outer, stride=SUB), :] for p in range(2)], axis=0
                    )
                )
            x = jnp.concatenate(cols, axis=1)
            high = x.astype(jnp.bfloat16)
            low = (x - high.astype(jnp.float32)).astype(jnp.bfloat16)
            mid = jnp.dot(
                first_v[...],
                jnp.concatenate([high, high, low], axis=0),
                preferred_element_type=jnp.float32,
            )
            turn_re, turn_im = turn_v[0], turn_v[1]
            turned = []
            for k in range(2):
                re = mid[:outer, k * LANES : (k + 1) * LANES]
                im = mid[outer:, k * LANES : (k + 1) * LANES]
                turned.append(
                    jnp.concatenate(
                        [re * turn_re - im * turn_im, re * turn_im + im * turn_re], axis=1
                    )
                )
            y = jnp.concatenate(turned, axis=0)
            high = y.astype(jnp.bfloat16)
            low = (y - high.astype(jnp.float32)).astype(jnp.bfloat16)
            out = lax.dot_general(
                second_v[...],
                jnp.concatenate([high, high, low], axis=1),
                (((1,), (1,)), ((), ())),
                preferred_element_type=jnp.float32,
            )
            flat = out_v.reshape(tiles, LANES * 2 * SUB, outer)
            for k in range(2):
                for p in range(2):
                    flat[t, pl.ds(p * SUB + i * 2 + k, LANES, stride=2 * SUB), :] = out[
                        p * LANES : (p + 1) * LANES, k * outer : (k + 1) * outer
                    ]
            return carry

        lax.fori_loop(begin // 2, stop // 2, pair, 0)

    def piece_send(j, d):
        t, begin, size = pieces[j]
        peer = lax.rem(band + d, nb)
        return pltpu.make_async_remote_copy(
            src_ref=out_v.at[t, pl.ds(peer * kept * 2, kept * 2), pl.ds(begin, size), :],
            dst_ref=recv_v.at[band * tiles + t, :, pl.ds(begin, size), :],
            send_sem=es_sem.at[j, d - 1],
            recv_sem=er_sem.at[j, d - 1],
            device_id=(chan, peer),
            device_id_type=MESH,
        )

    def slice_send(q, d):
        peer = lax.rem(band + d, nb)
        return pltpu.make_async_remote_copy(
            src_ref=out_v.at[pl.ds(early, late), pl.ds((peer * kept + q * span) * 2, span * 2)],
            dst_ref=recv_v.at[pl.ds(band * tiles + early, late), pl.ds(q * span * 2, span * 2)],
            send_sem=ls_sem.at[q, d - 1],
            recv_sem=lr_sem.at[q, d - 1],
            device_id=(chan, peer),
            device_id_type=MESH,
        )

    def keep(t):
        recv_v[band * tiles + t] = out_v[t, pl.ds(band * kept * 2, kept * 2)]

    def flip(q):
        def one(k, carry):
            for p in range(2):
                block = recv_v[:, q * span * 2 + k * 2 + p]
                spec_ref[p, 0, pl.ds(pl.multiple_of((q * span + k) * outer, LANES), outer), :] = block.reshape(
                    nb * tiles * SUB, outer
                ).T
            return carry

        lax.fori_loop(0, span, one, 0, unroll=2 if span % 2 == 0 else 1)

    def weigh(c):
        step = 512 if wide % 512 == 0 else LANES

        def one(j, carry):
            spot = 0
            for s in range(steps):
                spot = spot + ((j // (1 << s)) % 2) * (1 << (steps - 1 - s))
            for q in range(wide // step):
                col = pl.multiple_of((j * cuts + c % cuts) * wide + q * step, LANES)
                sums = [None] * 3
                for ch in range(count):
                    x = res_v[c // cuts, ch, :, pl.ds(col, step)]
                    for t in range(3):
                        term = coeffs[ch][t] * x
                        sums[t] = term if ch == 0 else sums[t] + term
                for t in range(3):
                    part_v[c, spot, pl.ds(t * SUB, SUB), pl.ds(q * step, step)] = sums[t]
            return carry

        lax.fori_loop(0, nc, one, 0)

    def half_send(c, s):
        size = nc >> (s + 1)
        begin = starts[s] + (1 - bits[s]) * size
        return pltpu.make_async_remote_copy(
            src_ref=part_v.at[c, pl.ds(begin, size)],
            dst_ref=lands[s].at[c],
            send_sem=rs_sem.at[c, s],
            recv_sem=rr_sem.at[c, s],
            device_id=(partners[s], band),
            device_id_type=MESH,
        )

    def mom_send(s):
        return pltpu.make_async_remote_copy(
            src_ref=mom_v.at[s],
            dst_ref=mom_land.at[s],
            send_sem=ms_sem.at[s],
            recv_sem=mr_sem.at[s],
            device_id=(partners[s], band),
            device_id_type=MESH,
        )

    solved = []

    def mom_add(s):
        mom_send(s).wait_recv()
        moment = mom_v[s] + mom_land[s]
        if s < steps - 1:
            mom_v[s + 1] = moment
            mom_send(s + 1).start()
            return
        for entry in inverse_rows(moment):
            solved.append(jnp.broadcast_to(entry, (SUB, LANES)))

    def half_add(c, s, send=True):
        half_send(c, s).wait_recv()
        size = nc >> (s + 1)
        if s == steps - 1:
            aa, ab, ac, bb, bc, cc = solved
            table = ((aa, ab, ac), (ab, bb, bc), (ac, bc, cc))
            for q in range(wide // LANES):
                at = pl.ds(q * LANES, LANES)
                tay = [
                    part_v[c, starts[s + 1], pl.ds(t * SUB, SUB), at] + lands[s][c, 0, pl.ds(t * SUB, SUB), at]
                    for t in range(3)
                ]
                for t, row in enumerate(table):
                    comp_ref[t, pl.ds(c // cuts * SUB, SUB), pl.ds(c % cuts * wide + q * LANES, LANES)] = (
                        row[0] * tay[0] + row[1] * tay[1] + row[2] * tay[2]
                    )
            return
        half = size // 2
        for mine in (1 - bits[s + 1], bits[s + 1]):
            for q in range(half):
                at = mine * half + q
                part_v[c, starts[s + 1] + at] = part_v[c, starts[s + 1] + at] + lands[s][c, at]
            if send and mine is not bits[s + 1]:
                half_send(c, s + 1).start()

    ahead = min(AHEAD, chunks)
    moved = weighed = added = 0

    def advance(target):
        nonlocal moved
        while moved < min(target, chunks):
            half_add(moved, 1)
            if moved + ahead < chunks:
                half_send(moved + ahead, 1).start()
            moved += 1

    def spread(target):
        nonlocal weighed
        while weighed < min(target, chunks):
            if weighed % cuts == 0:
                res_copy(weighed // cuts).wait()
            weigh(weighed)
            half_send(weighed, 0).start()
            weighed += 1

    def gather(target):
        nonlocal added
        while added < min(target, chunks):
            half_add(added, 0, send=added < ahead)
            added += 1

    for j in range(bases, -1, -1):
        table_copy(j).wait()
    grid_copy(0).wait()
    for i in range(max(tiles, parts)):
        if i < parts:
            res_copy(i).start()
        if 0 < i + 1 < tiles:
            grid_copy(i + 1).start()

    half = SUB // 2
    ends = {(t, begin + size): j for j, (t, begin, size) in enumerate(pieces)}
    for unit in range(2 * tiles):
        t, begin = unit // 2, unit % 2 * half
        if unit > 1 and begin == 0:
            grid_copy(t).wait()
        transform(t, begin, begin + half)
        if unit == 0:
            pl.semaphore_wait(barrier, nb - 1 + steps)
            mom_send(0).start()
        j = ends.get((t, begin + half))
        if j is not None:
            for d in range(1, nb):
                piece_send(j, d).start()
        if unit == 0:
            spread(1)
            mom_add(0)
            spread(3)
            gather(2)
        else:
            spread(3 * (unit + 1))
            gather(3 * (unit + 1) - 1)
            if unit == 2:
                mom_add(1)
            advance((0, 0, 1, 2, 3, 3, 4, 5)[min(unit, 7)])
        if begin:
            keep(t)
    for q in range(slices):
        for d in range(1, nb):
            slice_send(q, d).start()
    spread(chunks)
    gather(chunks)

    def open_pieces():
        for j in range(len(pieces)):
            for d in range(1, nb):
                piece_send(j, d).wait_recv()

    def flip_go(q):
        for d in range(1, nb):
            slice_send(q, d).wait_recv()
        flip(q)

    def z_due(c):
        return 7.2 + 38.0 * (c + 1) / chunks

    jobs = [(z_due(c), 1, advance, (c + 1,)) for c in range(moved, chunks)]
    for s in range(2, steps):
        jobs.append((z_due(0) + s, s, mom_add, (s,)))
        for c in range(chunks):
            jobs.append((max(z_due(c + 2 * (s - 1)) + 2.4, 45.5 + (s - steps)), s, half_add, (c, s)))
    jobs.append((28.0, 9, open_pieces, ()))
    for q in range(slices):
        jobs.append((32.0 + 22.5 * (q + 1) / slices, 10, flip_go, (q,)))
    jobs.sort(key=lambda job: job[:2])
    for _, _, work, args in jobs:
        work(*args)

    def drain_z():
        for s in range(steps):
            mom_send(s).wait_send()
        for c in range(chunks):
            for s in range(steps):
                half_send(c, s).wait_send()

    def drain_band():
        for d in range(1, nb):
            for j in range(len(pieces)):
                piece_send(j, d).wait_send()
            for q in range(slices):
                slice_send(q, d).wait_send()

    drain_z()
    drain_band()


def head_pieces(tiles):
    early = tiles // 2
    half = SUB // 2
    return [(0, 0, half), (0, half, half)][: 2 * early] + [(t, 0, SUB) for t in range(1, early)]


def place_kernel(spec_ref, comp_ref, spec_hbm, comp_hbm, sem):
    cuts = sem.shape[0] // 2
    rows = spec_ref.shape[2] // cuts
    copies = [pltpu.make_async_copy(comp_ref, comp_hbm, sem.at[2 * cuts])]
    for p in range(2):
        for k in range(cuts):
            at = (p, 0, pl.ds(k * rows, rows))
            copies.append(pltpu.make_async_copy(spec_ref.at[at], spec_hbm.at[at], sem.at[p * cuts + k]))
    for copy in copies:
        copy.start()
    for copy in copies:
        copy.wait()


def local(nc, nb, residual, weight_index, weight_table, gridded):
    count, row_count, columns = residual.shape
    _, groups, rows, length = gridded.shape
    outer = length // LANES
    tiles, parts = rows // SUB, row_count // SUB
    wide = columns // nc
    halves = 4
    kept = LANES // nb
    slices = min(8, kept)
    steps = int(math.log2(nc))
    view = gridded.reshape(2, tiles, SUB, outer, LANES)
    view = jnp.transpose(view, (0, 1, 3, 2, 4)).reshape(2, tiles, outer * SUB, LANES)
    vmem = pl.BlockSpec(memory_space=pltpu.VMEM)
    hbm = pl.BlockSpec(memory_space=pl.ANY)
    dma = pltpu.SemaphoreType.DMA
    consts = [jnp.asarray(table) for table in tables(length)]
    bases = len(consts) - 1
    pieces = len(head_pieces(tiles))
    shape_spec = (2, 1, kept * outer, nb * rows)
    shape_comp = (3, row_count, wide)
    held = pl.pallas_call(
        functools.partial(exchange_kernel, nc, nb, bases),
        out_shape=(pltpu.VMEM(shape_spec, jnp.float32), pltpu.VMEM(shape_comp, jnp.float32)),
        in_specs=[hbm] * (bases + 5),
        out_specs=(vmem, vmem),
        scratch_shapes=[
            *[pltpu.VMEM(c.shape, c.dtype) for c in consts],
            pltpu.SMEM(weight_index.shape, jnp.int32),
            pltpu.SMEM(weight_table.shape, jnp.float32),
            pltpu.VMEM((2, tiles, outer * SUB, LANES), jnp.float32),
            pltpu.VMEM((tiles, LANES * 2, SUB, outer), jnp.float32),
            pltpu.VMEM((nb * tiles, kept * 2, SUB, outer), jnp.float32),
            pltpu.VMEM((parts, count, SUB, columns), jnp.float32),
            pltpu.VMEM((parts * halves, nc, 3 * SUB, wide // halves), jnp.float32),
            pltpu.VMEM((steps, SUB, LANES), jnp.float32),
            pltpu.VMEM((steps, SUB, LANES), jnp.float32),
            *[
                pltpu.VMEM((parts * halves, nc >> (s + 1), 3 * SUB, wide // halves), jnp.float32)
                for s in range(steps)
            ],
            dma((2,)),
            dma((bases + 1,)),
            dma((tiles,)),
            dma((parts,)),
            dma((pieces, nb - 1)),
            dma((pieces, nb - 1)),
            dma((slices, nb - 1)),
            dma((slices, nb - 1)),
            dma((parts * halves, steps)),
            dma((parts * halves, steps)),
            dma((steps,)),
            dma((steps,)),
        ],
        compiler_params=pltpu.CompilerParams(
            collective_id=0, has_side_effects=True, vmem_limit_bytes=62_200_000
        ),
        name="exchange",
    )(weight_index, weight_table, *consts, residual, view)
    cuts = 4
    spectrum, components = pl.pallas_call(
        place_kernel,
        out_shape=(
            jax.ShapeDtypeStruct(shape_spec, jnp.float32),
            jax.ShapeDtypeStruct(shape_comp, jnp.float32),
        ),
        in_specs=[vmem, vmem],
        out_specs=(hbm, hbm),
        scratch_shapes=[dma((2 * cuts + 1,))],
        compiler_params=pltpu.CompilerParams(vmem_limit_bytes=16 * 1024 * 1024),
        name="place",
    )(*held)
    return (components, spectrum)


def solution(mesh):
    nc, nb = mesh.shape["chan"], mesh.shape["band"]
    in_specs = (P("chan", "band", None), P("chan"), P(), P(None, "chan", "band", None))
    out_specs = (P(None, "band", "chan"), P(None, "chan", "band", None))
    return jax.shard_map(
        functools.partial(local, nc, nb),
        mesh=mesh,
        in_specs=in_specs,
        out_specs=out_specs,
        check_vma=False,
    )
```

```python
import functools
import math

import jax
import jax.numpy as jnp
import numpy as np
from jax import lax
from jax.experimental import pallas as pl
from jax.experimental.pallas import tpu as pltpu
from jax.sharding import PartitionSpec as P

MESH = pl.DeviceIdType.MESH
LANES = 128
SUB = 8
AHEAD = 3


def block_form(table):
    real = np.block([[table.real, -table.imag], [table.imag, table.real]]).astype(np.float32)
    high = real.astype(jnp.bfloat16)
    low = (real - high.astype(np.float32)).astype(jnp.bfloat16)
    return np.concatenate([high, low, high], axis=1)


def dft(size):
    grid = np.outer(np.arange(size), np.arange(size)) % size
    return np.exp(-2j * np.pi * grid / size)


def tables(length):
    outer = length // LANES
    turn = np.exp(-2j * np.pi * np.outer(np.arange(outer), np.arange(LANES)) / length)
    turn = turn / math.sqrt(length)
    bases = [block_form(dft(outer))]
    if outer != LANES:
        bases.append(block_form(dft(LANES)))
    return (np.stack([turn.real, turn.imag]).astype(np.float32), *bases)


def inverse_rows(moment):
    s0, s1, s2, s3, s4 = (moment[j : j + 1, :] for j in range(5))
    aa = s2 * s4 - s3 * s3
    ab = s2 * s3 - s1 * s4
    ac = s1 * s3 - s2 * s2
    bb = s0 * s4 - s2 * s2
    bc = s1 * s2 - s0 * s3
    cc = s0 * s2 - s1 * s1
    determ = s0 * aa + s1 * ab + s2 * ac
    return [entry / determ for entry in (aa, ab, ac, bb, bc, cc)]


def exchange_kernel(nc, nb, bases, idx_hbm, tab_hbm, *rest):
    steps = int(math.log2(nc))
    tables_hbm, (res_hbm, grid_hbm) = rest[: bases + 1], rest[bases + 1 : bases + 3]
    spec_ref, comp_ref, recv_v = rest[bases + 3 : bases + 6]
    rest = rest[bases + 6 :]
    tables_v, rest = rest[: bases + 1], rest[bases + 1 :]
    (idx_ref, tab_ref, grid_v, out_v, res_v, part_v, mom_v, mom_land) = rest[:8]
    lands = rest[8 : 8 + steps]
    (idx_sem, tab_sem, grid_sem, res_sem, bs_sem, er_sem, lr_sem, rs_sem, rr_sem, ms_sem, mr_sem) = rest[8 + steps :]
    turn_v, first_v, second_v = tables_v[0], tables_v[1], tables_v[-1]
    chan = lax.axis_index("chan")
    band = lax.axis_index("band")
    tiles, outer8 = grid_v.shape[1], grid_v.shape[2]
    outer = outer8 // SUB
    kept = LANES // nb
    parts = res_v.shape[0]
    count = res_v.shape[1]
    wide = part_v.shape[3]
    chunks = part_v.shape[0]
    cuts = chunks // parts
    early = tiles // 2
    late = tiles - early
    pieces = head_pieces(tiles)
    slices = lr_sem.shape[0]
    span = kept // slices

    def table_copy(j):
        return pltpu.make_async_copy(tables_hbm[j], tables_v[j], tab_sem.at[j])

    def grid_copy(t):
        return pltpu.make_async_copy(grid_hbm.at[:, t], grid_v.at[:, t], grid_sem.at[t])

    def res_copy(c):
        return pltpu.make_async_copy(
            res_hbm.at[:, pl.ds(c * SUB, SUB), :], res_v.at[c], res_sem.at[c]
        )

    bits = [(chan // (1 << s)) % 2 for s in range(steps)]
    partners = [chan + (1 - 2 * bits[s]) * (1 << s) for s in range(steps)]
    others = [crossed(band, nb, mask) for mask in range(nb - 1, 0, -1)]
    starts = [0]
    for s in range(steps):
        starts.append(starts[s] + bits[s] * (nc >> (s + 1)))

    small = [
        pltpu.make_async_copy(idx_hbm, idx_ref, idx_sem.at[0]),
        pltpu.make_async_copy(tab_hbm, tab_ref, idx_sem.at[1]),
    ]
    for j in range(bases, -1, -1):
        table_copy(j).start()
    grid_copy(0).start()
    for copy in small:
        copy.start()

    barrier = pltpu.get_barrier_semaphore()
    for peer in others:
        pl.semaphore_signal(barrier, inc=1, device_id=(chan, peer), device_id_type=MESH)
    for s in range(steps):
        pl.semaphore_signal(barrier, inc=1, device_id=(partners[s], band), device_id_type=MESH)

    def transform(t, begin, stop):
        def pair(i, carry):
            cols = []
            for k in range(2):
                r = i * 2 + k
                cols.append(
                    jnp.concatenate(
                        [grid_v[p, t, pl.ds(r, outer, stride=SUB), :] for p in range(2)], axis=0
                    )
                )
            x = jnp.concatenate(cols, axis=1)
            high = x.astype(jnp.bfloat16)
            low = (x - high.astype(jnp.float32)).astype(jnp.bfloat16)
            mid = jnp.dot(
                first_v[...],
                jnp.concatenate([high, high, low], axis=0),
                preferred_element_type=jnp.float32,
            )
            turn_re, turn_im = turn_v[0], turn_v[1]
            turned = []
            for k in range(2):
                re = mid[:outer, k * LANES : (k + 1) * LANES]
                im = mid[outer:, k * LANES : (k + 1) * LANES]
                turned.append(
                    jnp.concatenate(
                        [re * turn_re - im * turn_im, re * turn_im + im * turn_re], axis=1
                    )
                )
            y = jnp.concatenate(turned, axis=0)
            high = y.astype(jnp.bfloat16)
            low = (y - high.astype(jnp.float32)).astype(jnp.bfloat16)
            out = lax.dot_general(
                second_v[...],
                jnp.concatenate([high, high, low], axis=1),
                (((1,), (1,)), ((), ())),
                preferred_element_type=jnp.float32,
            )
            flat = out_v.reshape(tiles, LANES * 2 * SUB, outer)
            for k in range(2):
                for p in range(2):
                    flat[t, pl.ds(p * SUB + i * 2 + k, LANES, stride=2 * SUB), :] = out[
                        p * LANES : (p + 1) * LANES, k * outer : (k + 1) * outer
                    ]
            return carry

        lax.fori_loop(begin // 2, stop // 2, pair, 0)

    def piece_send(j, peer):
        t, begin, size = pieces[j]
        return pltpu.make_async_remote_copy(
            src_ref=out_v.at[t, pl.ds(peer * kept * 2, kept * 2), pl.ds(begin, size), :],
            dst_ref=recv_v.at[band * tiles + t, :, pl.ds(begin, size), :],
            send_sem=bs_sem.at[0],
            recv_sem=er_sem.at[0],
            device_id=(chan, peer),
            device_id_type=MESH,
        )

    def slice_send(q, peer):
        return pltpu.make_async_remote_copy(
            src_ref=out_v.at[pl.ds(early, late), pl.ds((peer * kept + q * span) * 2, span * 2)],
            dst_ref=recv_v.at[pl.ds(band * tiles + early, late), pl.ds(q * span * 2, span * 2)],
            send_sem=bs_sem.at[0],
            recv_sem=lr_sem.at[q],
            device_id=(chan, peer),
            device_id_type=MESH,
        )

    def keep(t):
        recv_v[band * tiles + t] = out_v[t, pl.ds(band * kept * 2, kept * 2)]

    def flip(q):
        flip_slice(recv_v, spec_ref, q * span, span)

    coeffs = []

    def weigh(c):
        step = 512 if wide % 512 == 0 else LANES

        def one(j, carry):
            spot = 0
            for s in range(steps):
                spot = spot + ((j // (1 << s)) % 2) * (1 << (steps - 1 - s))
            for q in range(wide // step):
                col = pl.multiple_of((j * cuts + c % cuts) * wide + q * step, LANES)
                sums = [None] * 3
                for ch in range(count):
                    x = res_v[c // cuts, ch, :, pl.ds(col, step)]
                    for t in range(3):
                        term = coeffs[ch][t] * x
                        sums[t] = term if ch == 0 else sums[t] + term
                for t in range(3):
                    part_v[c, spot, pl.ds(t * SUB, SUB), pl.ds(q * step, step)] = sums[t]
            return carry

        lax.fori_loop(0, nc, one, 0)

    batches = batch_list(chunks, steps)

    def batch_of(c, s):
        for spot, (step, first, last) in enumerate(batches):
            if step == s and first <= c < last:
                return spot, first, last

    def landed(ref, sem):
        pltpu.make_async_copy(ref, ref, sem).wait()

    def half_send(c, s):
        size = nc >> (s + 1)
        begin = starts[s] + (1 - bits[s]) * size
        return pltpu.make_async_remote_copy(
            src_ref=part_v.at[c, pl.ds(begin, size)],
            dst_ref=lands[s].at[c],
            send_sem=rs_sem.at[0],
            recv_sem=rr_sem.at[batch_of(c, s)[0]],
            device_id=(partners[s], band),
            device_id_type=MESH,
        )

    def mom_send(s):
        return pltpu.make_async_remote_copy(
            src_ref=mom_v.at[s],
            dst_ref=mom_land.at[s],
            send_sem=ms_sem.at[0],
            recv_sem=mr_sem.at[s],
            device_id=(partners[s], band),
            device_id_type=MESH,
        )

    solved = []

    def mom_add(s):
        mom_send(s).wait_recv()
        moment = mom_v[s] + mom_land[s]
        if s < steps - 1:
            mom_v[s + 1] = moment
            mom_send(s + 1).start()
            return
        for entry in inverse_rows(moment):
            solved.append(jnp.broadcast_to(entry, (SUB, LANES)))

    def half_add(c, s, send=True):
        spot, first, last = batch_of(c, s)
        if c == first:
            landed(lands[s].at[pl.ds(first, last - first)], rr_sem.at[spot])
        size = nc >> (s + 1)
        if s == steps - 1:
            aa, ab, ac, bb, bc, cc = solved
            table = ((aa, ab, ac), (ab, bb, bc), (ac, bc, cc))
            for q in range(wide // LANES):
                at = pl.ds(q * LANES, LANES)
                tay = [
                    part_v[c, starts[s + 1], pl.ds(t * SUB, SUB), at] + lands[s][c, 0, pl.ds(t * SUB, SUB), at]
                    for t in range(3)
                ]
                for t, row in enumerate(table):
                    comp_ref[t, pl.ds(c // cuts * SUB, SUB), pl.ds(c % cuts * wide + q * LANES, LANES)] = (
                        row[0] * tay[0] + row[1] * tay[1] + row[2] * tay[2]
                    )
            return
        half = size // 2
        for mine in (1 - bits[s + 1], bits[s + 1]):
            for q in range(half):
                at = mine * half + q
                part_v[c, starts[s + 1] + at] = part_v[c, starts[s + 1] + at] + lands[s][c, at]
            if send and mine is not bits[s + 1]:
                half_send(c, s + 1).start()

    ahead = min(AHEAD, chunks)
    moved = weighed = added = 0
    issued = ahead

    def advance(target, ahead=AHEAD):
        nonlocal moved, issued
        while moved < min(target, chunks):
            half_add(moved, 1)
            moved += 1
            while issued < min(moved + ahead, chunks):
                half_send(issued, 1).start()
                issued += 1

    def spread(target):
        nonlocal weighed
        while weighed < min(target, chunks):
            if weighed % cuts == 0:
                res_copy(weighed // cuts).wait()
            weigh(weighed)
            half_send(weighed, 0).start()
            weighed += 1

    def gather(target):
        nonlocal added
        while added < min(target, chunks):
            half_add(added, 0, send=added < ahead)
            added += 1

    for j in range(bases, -1, -1):
        table_copy(j).wait()
    grid_copy(0).wait()
    for i in range(max(tiles, parts)):
        if i < parts:
            res_copy(i).start()
        if 0 < i + 1 < tiles:
            grid_copy(i + 1).start()

    for copy in small:
        copy.wait()
    total = count * nc
    moments = [jnp.float32(0.0)] * 5
    for c in range(count):
        weight = tab_ref[idx_ref[c]]
        position = (chan * count + c).astype(jnp.float32)
        offset = (2.0 * position + 1.0) * (1.0 / total) - 1.0
        power = weight
        trio = []
        for j in range(5):
            if j < 3:
                trio.append(power)
            moments[j] = moments[j] + power
            power = power * offset
        coeffs.append(trio)
    line = lax.broadcasted_iota(jnp.int32, (SUB, LANES), 0)
    tile = jnp.zeros((SUB, LANES), jnp.float32)
    for j in range(5):
        tile = jnp.where(line == j, moments[j], tile)
    mom_v[0] = tile

    half = SUB // 2
    goals = [last for step, _, last in batches if step == 0]
    ends = {(t, begin + size): j for j, (t, begin, size) in enumerate(pieces)}
    for unit in range(2 * tiles):
        t, begin = unit // 2, unit % 2 * half
        if unit > 1 and begin == 0:
            grid_copy(t).wait()
        transform(t, begin, begin + half)
        if unit == 0:
            pl.semaphore_wait(barrier, nb - 1 + steps)
            mom_send(0).start()
        j = ends.get((t, begin + half))
        if j is not None:
            for peer in others:
                piece_send(j, peer).start()
        if unit == 0:
            spread(goals[0])
            mom_add(0)
            spread(goals[1])
            gather(goals[1])
        else:
            gather(goals[min(unit, len(goals) - 1)])
            spread(goals[min(unit + 1, len(goals) - 1)])
            if unit == 2:
                mom_add(1)
            advance((0, 0, 1, 2, 3, 3, 4, 5)[min(unit, 7)])
        if begin:
            keep(t)
    for q in range(slices):
        for peer in others:
            slice_send(q, peer).start()
    spread(chunks)
    gather(chunks)

    def open_pieces():
        landed(recv_v.at[pl.ds(0, (nb - 1) * early)], er_sem.at[0])

    def flip_go(q):
        landed(recv_v.at[pl.ds(0, (nb - 1) * late), pl.ds(0, span * 2)], lr_sem.at[q])
        if q < slices - 1:
            flip(q)

    def z_due(c):
        return 7.2 + 38.0 * (c + 1) / chunks

    jobs = [(z_due(c), 1, advance, (c + 1, 2)) for c in range(moved, chunks)]
    for s in range(2, steps):
        jobs.append((z_due(0) + s, s, mom_add, (s,)))
        for c in range(chunks):
            jobs.append((max(z_due(c + 2 * (s - 1)) + 2.4, 45.5 + (s - steps)), s, half_add, (c, s)))
    jobs.append((28.0, 9, open_pieces, ()))
    for q in range(slices):
        jobs.append((32.0 + 22.5 * (q + 1) / slices, 10, flip_go, (q,)))
    jobs.sort(key=lambda job: job[:2])
    for _, _, work, args in jobs:
        work(*args)

    def drain_z():
        landed(mom_v, ms_sem.at[0])
        landed(part_v.at[:, pl.ds(0, nc - 1)], rs_sem.at[0])

    def drain_band():
        landed(recv_v.at[pl.ds(0, (nb - 1) * tiles)], bs_sem.at[0])

    drain_z()
    drain_band()


def crossed(index, size, mask):
    peer = 0
    for bit in range(int(math.log2(size))):
        own = (index // (1 << bit)) % 2
        peer = peer + (1 - own if mask >> bit & 1 else own) * (1 << bit)
    return peer


def flip_slice(recv_v, spec_ref, first, span):
    rows, outer = recv_v.shape[0] * SUB, recv_v.shape[3]

    def one(k, carry):
        for p in range(2):
            block = recv_v[:, (first + k) * 2 + p].reshape(rows, outer)
            spec_ref[p, 0, pl.ds(pl.multiple_of((first + k) * outer, LANES), outer), :] = block.T
        return carry

    lax.fori_loop(0, span, one, 0, unroll=2 if span % 2 == 0 else 1)


def batch_list(chunks, steps):
    batches = [(0, 0, 1), (0, 1, min(3, chunks))]
    batches += [(0, c, min(c + 3, chunks)) for c in range(3, chunks, 3)]
    for s in range(1, steps - 1):
        batches += [(s, c, c + 1) for c in range(chunks)]
    cuts = sorted({0, max(chunks - 4, 0), chunks - 1, chunks})
    return batches + [(steps - 1, a, b) for a, b in zip(cuts, cuts[1:])]


def head_pieces(tiles):
    early = tiles // 2
    half = SUB // 2
    return [(0, 0, half), (0, half, half)][: 2 * early] + [(t, 0, SUB) for t in range(1, early)]


def place_kernel(slices, spec_ref, comp_ref, recv_ref, spec_hbm, comp_hbm, spec_v, sem):
    rows = spec_ref.shape[2] // slices
    ready = rows * (slices - 1)
    span = recv_ref.shape[1] // 2 // slices
    copies = [
        pltpu.make_async_copy(spec_ref.at[p, 0, pl.ds(0, ready)], spec_hbm.at[p, 0, pl.ds(0, ready)], sem.at[p])
        for p in range(2)
    ]
    copies.append(pltpu.make_async_copy(comp_ref, comp_hbm, sem.at[2]))
    for copy in copies:
        copy.start()
    many, outer = recv_ref.shape[0] * SUB, recv_ref.shape[3]
    for k in range(span):
        for p in range(2):
            block = recv_ref[:, (span * (slices - 1) + k) * 2 + p].reshape(many, outer)
            spec_v[p, pl.ds(k * outer, outer), :] = block.T
    copies.append(pltpu.make_async_copy(spec_v, spec_hbm.at[:, 0, pl.ds(ready, rows)], sem.at[3]))
    copies[-1].start()
    for copy in copies:
        copy.wait()


def local(nc, nb, residual, weight_index, weight_table, gridded):
    count, row_count, columns = residual.shape
    _, groups, rows, length = gridded.shape
    outer = length // LANES
    tiles, parts = rows // SUB, row_count // SUB
    wide = columns // nc
    halves = 4
    kept = LANES // nb
    slices = min(8, kept)
    steps = int(math.log2(nc))
    view = gridded.reshape(2, tiles, SUB, outer, LANES)
    view = jnp.transpose(view, (0, 1, 3, 2, 4)).reshape(2, tiles, outer * SUB, LANES)
    vmem = pl.BlockSpec(memory_space=pltpu.VMEM)
    hbm = pl.BlockSpec(memory_space=pl.ANY)
    dma = pltpu.SemaphoreType.DMA
    consts = [jnp.asarray(table) for table in tables(length)]
    bases = len(consts) - 1
    shape_spec = (2, 1, kept * outer, nb * rows)
    shape_comp = (3, row_count, wide)
    shape_recv = (nb * tiles, kept * 2, SUB, outer)
    batches = len(batch_list(parts * halves, steps))
    held = pl.pallas_call(
        functools.partial(exchange_kernel, nc, nb, bases),
        out_shape=tuple(pltpu.VMEM(shape, jnp.float32) for shape in (shape_spec, shape_comp, shape_recv)),
        in_specs=[hbm] * (bases + 5),
        out_specs=(vmem, vmem, vmem),
        scratch_shapes=[
            *[pltpu.VMEM(c.shape, c.dtype) for c in consts],
            pltpu.SMEM(weight_index.shape, jnp.int32),
            pltpu.SMEM(weight_table.shape, jnp.float32),
            pltpu.VMEM((2, tiles, outer * SUB, LANES), jnp.float32),
            pltpu.VMEM((tiles, LANES * 2, SUB, outer), jnp.float32),
            pltpu.VMEM((parts, count, SUB, columns), jnp.float32),
            pltpu.VMEM((parts * halves, nc, 3 * SUB, wide // halves), jnp.float32),
            pltpu.VMEM((steps, SUB, LANES), jnp.float32),
            pltpu.VMEM((steps, SUB, LANES), jnp.float32),
            *[
                pltpu.VMEM((parts * halves, nc >> (s + 1), 3 * SUB, wide // halves), jnp.float32)
                for s in range(steps)
            ],
            dma((2,)),
            dma((bases + 1,)),
            dma((tiles,)),
            dma((parts,)),
            dma((1,)),
            dma((1,)),
            dma((slices,)),
            dma((1,)),
            dma((batches,)),
            dma((1,)),
            dma((steps,)),
        ],
        compiler_params=pltpu.CompilerParams(
            collective_id=0, has_side_effects=True, vmem_limit_bytes=58_000_000
        ),
        name="exchange",
    )(weight_index, weight_table, *consts, residual, view)
    spectrum, components = pl.pallas_call(
        functools.partial(place_kernel, slices),
        out_shape=(
            jax.ShapeDtypeStruct(shape_spec, jnp.float32),
            jax.ShapeDtypeStruct(shape_comp, jnp.float32),
        ),
        in_specs=[vmem, vmem, vmem],
        out_specs=(hbm, hbm),
        scratch_shapes=[
            pltpu.VMEM((2, kept * outer // slices, nb * rows), jnp.float32),
            dma((4,)),
        ],
        compiler_params=pltpu.CompilerParams(vmem_limit_bytes=16 * 1024 * 1024),
        name="place",
    )(*held)
    return (components, spectrum)


def solution(mesh):
    nc, nb = mesh.shape["chan"], mesh.shape["band"]
    in_specs = (P("chan", "band", None), P("chan"), P(), P(None, "chan", "band", None))
    out_specs = (P(None, "band", "chan"), P(None, "chan", "band", None))
    return jax.shard_map(
        functools.partial(local, nc, nb),
        mesh=mesh,
        in_specs=in_specs,
        out_specs=out_specs,
        check_vma=False,
    )
```

```python
import functools
import math

import jax
import jax.numpy as jnp
import numpy as np
from jax import lax
from jax.experimental import pallas as pl
from jax.experimental.pallas import tpu as pltpu
from jax.sharding import PartitionSpec as P

MESH = pl.DeviceIdType.MESH
LANES = 128
SUB = 8
AHEAD = 3
HEAD = 2


def block_form(table):
    real = np.block([[table.real, -table.imag], [table.imag, table.real]]).astype(np.float32)
    high = real.astype(jnp.bfloat16)
    low = (real - high.astype(np.float32)).astype(jnp.bfloat16)
    return np.concatenate([high, low, high], axis=1)


def dft(size):
    grid = np.outer(np.arange(size), np.arange(size)) % size
    return np.exp(-2j * np.pi * grid / size)


def tables(length):
    outer = length // LANES
    turn = np.exp(-2j * np.pi * np.outer(np.arange(outer), np.arange(LANES)) / length)
    turn = turn / math.sqrt(length)
    bases = [block_form(dft(outer))]
    if outer != LANES:
        bases.append(block_form(dft(LANES)))
    return (np.stack([turn.real, turn.imag]).astype(np.float32), *bases)


def inverse_rows(moment):
    s0, s1, s2, s3, s4 = (moment[j : j + 1, :] for j in range(5))
    aa = s2 * s4 - s3 * s3
    ab = s2 * s3 - s1 * s4
    ac = s1 * s3 - s2 * s2
    bb = s0 * s4 - s2 * s2
    bc = s1 * s2 - s0 * s3
    cc = s0 * s2 - s1 * s1
    determ = s0 * aa + s1 * ab + s2 * ac
    return [entry / determ for entry in (aa, ab, ac, bb, bc, cc)]


def exchange_kernel(nc, nb, bases, idx_hbm, tab_hbm, *rest):
    steps = int(math.log2(nc))
    tables_hbm, (res_hbm, grid_hbm) = rest[: bases + 1], rest[bases + 1 : bases + 3]
    spec_ref, comp_ref, recv_v = rest[bases + 3 : bases + 6]
    rest = rest[bases + 6 :]
    tables_v, rest = rest[: bases + 1], rest[bases + 1 :]
    (idx_ref, tab_ref, grid_v, out_v, res_v, part_v, mom_v, mom_land) = rest[:8]
    lands = rest[8 : 8 + steps]
    (idx_sem, tab_sem, grid_sem, res_sem, bs_sem, er_sem, lr_sem, rs_sem, rr_sem, ms_sem, mr_sem) = rest[8 + steps :]
    turn_v, first_v, second_v = tables_v[0], tables_v[1], tables_v[-1]
    chan = lax.axis_index("chan")
    band = lax.axis_index("band")
    tiles, outer = grid_v.shape[1], grid_v.shape[2]
    kept = LANES // nb
    count, parts = res_v.shape[0], res_v.shape[1]
    wide = part_v.shape[3]
    chunks = part_v.shape[0]
    cuts = chunks // parts
    early = tiles // 2
    late = tiles - early
    pieces = head_pieces(tiles)
    slices = lr_sem.shape[0]
    span = kept // slices

    def table_copy(j):
        return pltpu.make_async_copy(tables_hbm[j], tables_v[j], tab_sem.at[j])

    def grid_copy(j):
        first, count, begin, size = grid_reads(tiles)[j]
        at = (slice(None), pl.ds(first, count), slice(None), pl.ds(begin, size))
        return pltpu.make_async_copy(grid_hbm.at[at], grid_v.at[at], grid_sem.at[j])

    def res_copy(j):
        first, count = res_reads(parts)[j]
        at = pl.ds(first, count)
        return pltpu.make_async_copy(res_hbm.at[:, at], res_v.at[:, at], res_sem.at[j])

    bits = [(chan // (1 << s)) % 2 for s in range(steps)]
    partners = [chan + (1 - 2 * bits[s]) * (1 << s) for s in range(steps)]
    others = [crossed(band, nb, mask) for mask in range(nb - 1, 0, -1)]
    starts = [0]
    for s in range(steps):
        starts.append(starts[s] + bits[s] * (nc >> (s + 1)))

    small = [
        pltpu.make_async_copy(idx_hbm, idx_ref, idx_sem.at[0]),
        pltpu.make_async_copy(tab_hbm, tab_ref, idx_sem.at[1]),
    ]
    for j in range(bases, -1, -1):
        table_copy(j).start()
    grid_copy(0).start()
    for copy in small:
        copy.start()

    barrier = pltpu.get_barrier_semaphore()
    for peer in others:
        pl.semaphore_signal(barrier, inc=1, device_id=(chan, peer), device_id_type=MESH)
    for s in range(steps):
        pl.semaphore_signal(barrier, inc=1, device_id=(partners[s], band), device_id_type=MESH)

    def transform(t, begin, stop):
        def pair(i, carry):
            grid_flat = grid_v.reshape(2, tiles, outer * SUB, LANES)
            cols = []
            for k in range(2):
                r = i * 2 + k
                cols.append(
                    jnp.concatenate(
                        [grid_flat[p, t, pl.ds(r, outer, stride=SUB), :] for p in range(2)], axis=0
                    )
                )
            x = jnp.concatenate(cols, axis=1)
            high = x.astype(jnp.bfloat16)
            low = (x - high.astype(jnp.float32)).astype(jnp.bfloat16)
            mid = jnp.dot(
                first_v[...],
                jnp.concatenate([high, high, low], axis=0),
                preferred_element_type=jnp.float32,
            )
            turn_re, turn_im = turn_v[0], turn_v[1]
            turned = []
            for k in range(2):
                re = mid[:outer, k * LANES : (k + 1) * LANES]
                im = mid[outer:, k * LANES : (k + 1) * LANES]
                turned.append(
                    jnp.concatenate(
                        [re * turn_re - im * turn_im, re * turn_im + im * turn_re], axis=1
                    )
                )
            y = jnp.concatenate(turned, axis=0)
            high = y.astype(jnp.bfloat16)
            low = (y - high.astype(jnp.float32)).astype(jnp.bfloat16)
            out = lax.dot_general(
                second_v[...],
                jnp.concatenate([high, high, low], axis=1),
                (((1,), (1,)), ((), ())),
                preferred_element_type=jnp.float32,
            )
            flat = out_v.reshape(tiles, LANES * 2 * SUB, outer)
            for k in range(2):
                for p in range(2):
                    flat[t, pl.ds(p * SUB + i * 2 + k, LANES, stride=2 * SUB), :] = out[
                        p * LANES : (p + 1) * LANES, k * outer : (k + 1) * outer
                    ]
            return carry

        lax.fori_loop(begin // 2, stop // 2, pair, 0)

    def piece_send(j, peer):
        t, begin, size = pieces[j]
        return pltpu.make_async_remote_copy(
            src_ref=out_v.at[t, pl.ds(peer * kept * 2, kept * 2), pl.ds(begin, size), :],
            dst_ref=recv_v.at[band * tiles + t, :, pl.ds(begin, size), :],
            send_sem=bs_sem.at[0],
            recv_sem=er_sem.at[0],
            device_id=(chan, peer),
            device_id_type=MESH,
        )

    def slice_send(q, peer):
        return pltpu.make_async_remote_copy(
            src_ref=out_v.at[pl.ds(early, late), pl.ds((peer * kept + q * span) * 2, span * 2)],
            dst_ref=recv_v.at[pl.ds(band * tiles + early, late), pl.ds(q * span * 2, span * 2)],
            send_sem=bs_sem.at[0],
            recv_sem=lr_sem.at[q],
            device_id=(chan, peer),
            device_id_type=MESH,
        )

    def keep(t):
        recv_v[band * tiles + t] = out_v[t, pl.ds(band * kept * 2, kept * 2)]

    def flip(q):
        flip_slice(recv_v, spec_ref, q * span, span)

    coeffs = []

    def weigh(c):
        step = 512 if wide % 512 == 0 else LANES

        def one(j, carry):
            spot = 0
            for s in range(steps):
                spot = spot + ((j // (1 << s)) % 2) * (1 << (steps - 1 - s))
            for q in range(wide // step):
                col = pl.multiple_of((j * cuts + c % cuts) * wide + q * step, LANES)
                sums = [None] * 3
                for ch in range(count):
                    x = res_v[ch, c // cuts, :, pl.ds(col, step)]
                    for t in range(3):
                        term = coeffs[ch][t] * x
                        sums[t] = term if ch == 0 else sums[t] + term
                for t in range(3):
                    part_v[c, spot, pl.ds(t * SUB, SUB), pl.ds(q * step, step)] = sums[t]
            return carry

        lax.fori_loop(0, nc, one, 0)

    batches = batch_list(chunks, steps)

    def batch_of(c, s):
        for spot, (step, first, last) in enumerate(batches):
            if step == s and first <= c < last:
                return spot, first, last

    def landed(ref, sem):
        pltpu.make_async_copy(ref, ref, sem).wait()

    def half_send(c, s):
        size = nc >> (s + 1)
        begin = starts[s] + (1 - bits[s]) * size
        return pltpu.make_async_remote_copy(
            src_ref=part_v.at[c, pl.ds(begin, size)],
            dst_ref=lands[s].at[c],
            send_sem=rs_sem.at[0],
            recv_sem=rr_sem.at[batch_of(c, s)[0]],
            device_id=(partners[s], band),
            device_id_type=MESH,
        )

    def mom_send(s):
        return pltpu.make_async_remote_copy(
            src_ref=mom_v.at[s],
            dst_ref=mom_land.at[s],
            send_sem=ms_sem.at[0],
            recv_sem=mr_sem.at[s],
            device_id=(partners[s], band),
            device_id_type=MESH,
        )

    solved = []

    def mom_add(s):
        mom_send(s).wait_recv()
        moment = mom_v[s] + mom_land[s]
        if s < steps - 1:
            mom_v[s + 1] = moment
            mom_send(s + 1).start()
            return
        for entry in inverse_rows(moment):
            solved.append(jnp.broadcast_to(entry, (SUB, LANES)))

    def half_add(c, s, send=True):
        spot, first, last = batch_of(c, s)
        if c == first:
            landed(lands[s].at[pl.ds(first, last - first)], rr_sem.at[spot])
        size = nc >> (s + 1)
        if s == steps - 1:
            aa, ab, ac, bb, bc, cc = solved
            table = ((aa, ab, ac), (ab, bb, bc), (ac, bc, cc))
            for q in range(wide // LANES):
                at = pl.ds(q * LANES, LANES)
                tay = [
                    part_v[c, starts[s + 1], pl.ds(t * SUB, SUB), at] + lands[s][c, 0, pl.ds(t * SUB, SUB), at]
                    for t in range(3)
                ]
                for t, row in enumerate(table):
                    comp_ref[t, pl.ds(c // cuts * SUB, SUB), pl.ds(c % cuts * wide + q * LANES, LANES)] = (
                        row[0] * tay[0] + row[1] * tay[1] + row[2] * tay[2]
                    )
            return
        half = size // 2
        for mine in (1 - bits[s + 1], bits[s + 1]):
            for q in range(half):
                at = mine * half + q
                part_v[c, starts[s + 1] + at] = part_v[c, starts[s + 1] + at] + lands[s][c, at]
            if send and mine is not bits[s + 1]:
                half_send(c, s + 1).start()

    ahead = min(AHEAD, chunks)
    moved = weighed = added = 0
    issued = ahead

    def advance(target, ahead=AHEAD):
        nonlocal moved, issued
        while moved < min(target, chunks):
            half_add(moved, 1)
            moved += 1
            while issued < min(moved + ahead, chunks):
                half_send(issued, 1).start()
                issued += 1

    def spread(target):
        nonlocal weighed
        while weighed < min(target, chunks):
            for j, (first, _) in enumerate(res_reads(parts)):
                if weighed == first * cuts:
                    res_copy(j).wait()
            weigh(weighed)
            half_send(weighed, 0).start()
            weighed += 1

    def gather(target):
        nonlocal added
        while added < min(target, chunks):
            half_add(added, 0, send=added < ahead)
            added += 1

    for j in range(bases, -1, -1):
        table_copy(j).wait()
    grid_copy(0).wait()
    grids, reads = len(grid_reads(tiles)), len(res_reads(parts))
    for j in range(max(grids - 1, reads)):
        if j + 1 < grids:
            grid_copy(j + 1).start()
        if j < reads:
            res_copy(j).start()

    for copy in small:
        copy.wait()
    total = count * nc
    moments = [jnp.float32(0.0)] * 5
    for c in range(count):
        weight = tab_ref[idx_ref[c]]
        position = (chan * count + c).astype(jnp.float32)
        offset = (2.0 * position + 1.0) * (1.0 / total) - 1.0
        power = weight
        trio = []
        for j in range(5):
            if j < 3:
                trio.append(power)
            moments[j] = moments[j] + power
            power = power * offset
        coeffs.append(trio)
    line = lax.broadcasted_iota(jnp.int32, (SUB, LANES), 0)
    tile = jnp.zeros((SUB, LANES), jnp.float32)
    for j in range(5):
        tile = jnp.where(line == j, moments[j], tile)
    mom_v[0] = tile

    half = SUB // 2
    goals = [last for step, _, last in batches if step == 0]
    ends = {(t, begin + size): j for j, (t, begin, size) in enumerate(pieces)}
    for unit in range(2 * tiles):
        t, begin = unit // 2, unit % 2 * half
        if unit == 2:
            for j in range(2, grids):
                grid_copy(j).wait()
        for top in range(begin, begin + half, HEAD if unit == 0 else half):
            stop = top + (HEAD if unit == 0 else half)
            if unit == 0 and top == HEAD:
                grid_copy(1).wait()
            transform(t, top, stop)
            if unit == 0 and top == 0:
                pl.semaphore_wait(barrier, nb - 1 + steps)
                mom_send(0).start()
            j = ends.get((t, stop))
            if j is not None:
                for peer in others:
                    piece_send(j, peer).start()
        if unit == 0:
            spread(goals[0])
            mom_add(0)
            spread(goals[1])
            gather(goals[1])
        else:
            gather(goals[min(unit, len(goals) - 1)])
            spread(goals[min(unit + 1, len(goals) - 1)])
            if unit == 2:
                mom_add(1)
            advance((0, 0, 1, 2, 3, 3, 4, 5)[min(unit, 7)])
        if begin:
            keep(t)
    for q in range(slices):
        for peer in others:
            slice_send(q, peer).start()
    spread(chunks)
    gather(chunks)

    def open_pieces():
        landed(recv_v.at[pl.ds(0, (nb - 1) * early)], er_sem.at[0])

    def flip_go(q):
        landed(recv_v.at[pl.ds(0, (nb - 1) * late), pl.ds(0, span * 2)], lr_sem.at[q])
        if q < slices - 1:
            flip(q)

    def z_due(c):
        return 7.2 + 38.0 * (c + 1) / chunks

    jobs = [(z_due(c), 1, advance, (c + 1, 2)) for c in range(moved, chunks)]
    for s in range(2, steps):
        jobs.append((z_due(0) + s, s, mom_add, (s,)))
        for c in range(chunks):
            due = z_due(chunks - 1) - 0.2 if s == steps - 1 else z_due(c)
            due += 1.5 * (s - 1) + 2.5 * (c == chunks - 1)
            jobs.append((due, s, half_add, (c, s)))
    jobs.append((28.0, 9, open_pieces, ()))
    for q in range(slices):
        jobs.append((32.0 + 22.5 * (q + 1) / slices, 10, flip_go, (q,)))
    jobs.sort(key=lambda job: job[:2])
    for _, _, work, args in jobs:
        work(*args)

    def drain_z():
        landed(mom_v, ms_sem.at[0])
        landed(part_v.at[:, pl.ds(0, nc - 1)], rs_sem.at[0])

    def drain_band():
        landed(recv_v.at[pl.ds(0, (nb - 1) * tiles)], bs_sem.at[0])

    drain_z()
    drain_band()


def crossed(index, size, mask):
    peer = 0
    for bit in range(int(math.log2(size))):
        own = (index // (1 << bit)) % 2
        peer = peer + (1 - own if mask >> bit & 1 else own) * (1 << bit)
    return peer


def flip_slice(recv_v, spec_ref, first, span):
    rows, outer = recv_v.shape[0] * SUB, recv_v.shape[3]

    def one(k, carry):
        for p in range(2):
            block = recv_v[:, (first + k) * 2 + p].reshape(rows, outer)
            spec_ref[p, 0, pl.ds(pl.multiple_of((first + k) * outer, LANES), outer), :] = block.T
        return carry

    lax.fori_loop(0, span, one, 0, unroll=2 if span % 2 == 0 else 1)


def batch_list(chunks, steps):
    batches = [(0, 0, 1), (0, 1, min(3, chunks))]
    batches += [(0, c, min(c + 3, chunks)) for c in range(3, chunks, 3)]
    for s in range(1, steps - 1):
        batches += [(s, c, c + 1) for c in range(chunks)]
    cuts = sorted({0, max(chunks - 4, 0), chunks - 1, chunks})
    return batches + [(steps - 1, a, b) for a, b in zip(cuts, cuts[1:])]


def head_pieces(tiles):
    early = tiles // 2
    half = SUB // 2
    first = [(0, top, HEAD) for top in range(0, half, HEAD)] + [(0, half, half)]
    return (first if early else []) + [(t, 0, SUB) for t in range(1, early)]


def grid_reads(tiles):
    reads = [(0, 1, 0, HEAD), (0, 1, HEAD, SUB - HEAD)]
    return reads + [(1, tiles - 1, 0, SUB)] * (tiles > 1)


def res_reads(parts):
    return [(0, 1)] + [(1, parts - 1)] * (parts > 1)


def place_kernel(slices, spec_ref, comp_ref, recv_ref, spec_hbm, comp_hbm, spec_v, sem):
    rows = spec_ref.shape[2] // slices
    ready = rows * (slices - 1)
    span = recv_ref.shape[1] // 2 // slices
    copies = [
        pltpu.make_async_copy(spec_ref.at[p, 0, pl.ds(0, ready)], spec_hbm.at[p, 0, pl.ds(0, ready)], sem.at[p])
        for p in range(2)
    ]
    copies.append(pltpu.make_async_copy(comp_ref, comp_hbm, sem.at[2]))
    for copy in copies:
        copy.start()
    many, outer = recv_ref.shape[0] * SUB, recv_ref.shape[3]
    for k in range(span):
        for p in range(2):
            block = recv_ref[:, (span * (slices - 1) + k) * 2 + p].reshape(many, outer)
            spec_v[p, pl.ds(k * outer, outer), :] = block.T
    copies.append(pltpu.make_async_copy(spec_v, spec_hbm.at[:, 0, pl.ds(ready, rows)], sem.at[3]))
    copies[-1].start()
    for copy in copies:
        copy.wait()


def local(nc, nb, residual, weight_index, weight_table, gridded):
    count, row_count, columns = residual.shape
    _, groups, rows, length = gridded.shape
    outer = length // LANES
    tiles, parts = rows // SUB, row_count // SUB
    wide = columns // nc
    halves = 4
    kept = LANES // nb
    slices = min(8, kept)
    steps = int(math.log2(nc))
    view = gridded.reshape(2, tiles, SUB, outer, LANES)
    view = jnp.transpose(view, (0, 1, 3, 2, 4))
    vmem = pl.BlockSpec(memory_space=pltpu.VMEM)
    hbm = pl.BlockSpec(memory_space=pl.ANY)
    dma = pltpu.SemaphoreType.DMA
    consts = [jnp.asarray(table) for table in tables(length)]
    bases = len(consts) - 1
    shape_spec = (2, 1, kept * outer, nb * rows)
    shape_comp = (3, row_count, wide)
    shape_recv = (nb * tiles, kept * 2, SUB, outer)
    batches = len(batch_list(parts * halves, steps))
    held = pl.pallas_call(
        functools.partial(exchange_kernel, nc, nb, bases),
        out_shape=tuple(pltpu.VMEM(shape, jnp.float32) for shape in (shape_spec, shape_comp, shape_recv)),
        in_specs=[hbm] * (bases + 5),
        out_specs=(vmem, vmem, vmem),
        scratch_shapes=[
            *[pltpu.VMEM(c.shape, c.dtype) for c in consts],
            pltpu.SMEM(weight_index.shape, jnp.int32),
            pltpu.SMEM(weight_table.shape, jnp.float32),
            pltpu.VMEM((2, tiles, outer, SUB, LANES), jnp.float32),
            pltpu.VMEM((tiles, LANES * 2, SUB, outer), jnp.float32),
            pltpu.VMEM((count, parts, SUB, columns), jnp.float32),
            pltpu.VMEM((parts * halves, nc, 3 * SUB, wide // halves), jnp.float32),
            pltpu.VMEM((steps, SUB, LANES), jnp.float32),
            pltpu.VMEM((steps, SUB, LANES), jnp.float32),
            *[
                pltpu.VMEM((parts * halves, nc >> (s + 1), 3 * SUB, wide // halves), jnp.float32)
                for s in range(steps)
            ],
            dma((2,)),
            dma((bases + 1,)),
            dma((len(grid_reads(tiles)),)),
            dma((len(res_reads(parts)),)),
            dma((1,)),
            dma((1,)),
            dma((slices,)),
            dma((1,)),
            dma((batches,)),
            dma((1,)),
            dma((steps,)),
        ],
        compiler_params=pltpu.CompilerParams(
            collective_id=0, has_side_effects=True, vmem_limit_bytes=58_000_000
        ),
        name="exchange",
    )(weight_index, weight_table, *consts, residual.reshape(count, parts, SUB, columns), view)
    spectrum, components = pl.pallas_call(
        functools.partial(place_kernel, slices),
        out_shape=(
            jax.ShapeDtypeStruct(shape_spec, jnp.float32),
            jax.ShapeDtypeStruct(shape_comp, jnp.float32),
        ),
        in_specs=[vmem, vmem, vmem],
        out_specs=(hbm, hbm),
        scratch_shapes=[
            pltpu.VMEM((2, kept * outer // slices, nb * rows), jnp.float32),
            dma((4,)),
        ],
        compiler_params=pltpu.CompilerParams(vmem_limit_bytes=16 * 1024 * 1024),
        name="place",
    )(*held)
    return (components, spectrum)


def solution(mesh):
    nc, nb = mesh.shape["chan"], mesh.shape["band"]
    in_specs = (P("chan", "band", None), P("chan"), P(), P(None, "chan", "band", None))
    out_specs = (P(None, "band", "chan"), P(None, "chan", "band", None))
    return jax.shard_map(
        functools.partial(local, nc, nb),
        mesh=mesh,
        in_specs=in_specs,
        out_specs=out_specs,
        check_vma=False,
    )
```

```python
import functools
import math

import jax
import jax.numpy as jnp
import numpy as np
from jax import lax
from jax.experimental import pallas as pl
from jax.experimental.pallas import tpu as pltpu
from jax.sharding import PartitionSpec as P

MESH = pl.DeviceIdType.MESH
LANES = 128
SUB = 8
HEAD = 2


def block_form(table):
    real = np.block([[table.real, -table.imag], [table.imag, table.real]]).astype(np.float32)
    high = real.astype(jnp.bfloat16)
    low = (real - high.astype(np.float32)).astype(jnp.bfloat16)
    return np.concatenate([high, low, high], axis=1)


def dft(size):
    grid = np.outer(np.arange(size), np.arange(size)) % size
    return np.exp(-2j * np.pi * grid / size)


def tables(length):
    outer = length // LANES
    turn = np.exp(-2j * np.pi * np.outer(np.arange(outer), np.arange(LANES)) / length)
    turn = turn / math.sqrt(length)
    bases = [block_form(dft(outer))]
    if outer != LANES:
        bases.append(block_form(dft(LANES)))
    return (np.stack([turn.real, turn.imag]).astype(np.float32), *bases)


def inverse_rows(moment):
    s0, s1, s2, s3, s4 = (moment[j : j + 1, :] for j in range(5))
    aa = s2 * s4 - s3 * s3
    ab = s2 * s3 - s1 * s4
    ac = s1 * s3 - s2 * s2
    bb = s0 * s4 - s2 * s2
    bc = s1 * s2 - s0 * s3
    cc = s0 * s2 - s1 * s1
    determ = s0 * aa + s1 * ab + s2 * ac
    return [entry / determ for entry in (aa, ab, ac, bb, bc, cc)]


def exchange_kernel(nc, nb, bases, idx_hbm, tab_hbm, *rest):
    line = nc // 2
    tables_hbm, (res_hbm, grid_hbm) = rest[: bases + 1], rest[bases + 1 : bases + 3]
    spec_ref, comp_ref, recv_v = rest[bases + 3 : bases + 6]
    rest = rest[bases + 6 :]
    tables_v, rest = rest[: bases + 1], rest[bases + 1 :]
    (idx_ref, tab_ref, grid_v, out_v, res_v, part_v, pair_v, land_v, mom_v, mom_land) = rest[:10]
    (idx_sem, tab_sem, grid_sem, res_sem, bs_sem, er_sem, lr_sem) = rest[10:17]
    (zs_sem, pair_sem, fw_sem, fin_sem, ms_sem, mr_sem, ok_sem) = rest[17:]
    turn_v, first_v, second_v = tables_v[0], tables_v[1], tables_v[-1]
    chan = lax.axis_index("chan")
    band = lax.axis_index("band")
    tiles, outer = grid_v.shape[1], grid_v.shape[2]
    kept = LANES // nb
    count, parts = res_v.shape[0], res_v.shape[1]
    wide = part_v.shape[3]
    cells = chunk_list(parts, wide)
    chunks = len(cells)
    early = tiles // 2
    late = tiles - early
    pieces = head_pieces(tiles)
    slices = lr_sem.shape[0]
    span = kept // slices

    def table_copy(j):
        return pltpu.make_async_copy(tables_hbm[j], tables_v[j], tab_sem.at[j])

    def grid_copy(j):
        first, count, begin, size = grid_reads(tiles)[j]
        at = (slice(None), pl.ds(first, count), slice(None), pl.ds(begin, size))
        return pltpu.make_async_copy(grid_hbm.at[at], grid_v.at[at], grid_sem.at[j])

    def res_copy(j):
        first, many, begin, size = res_reads(parts, wide)[j]
        at = (slice(None), pl.ds(first, many), slice(None), pl.ds(begin // LANES, size // LANES))
        return pltpu.make_async_copy(res_hbm.at[at], res_v.at[at], res_sem.at[j])

    core, place = chan % 2, chan // 2
    mate = chan + 1 - 2 * core
    others = [crossed(band, nb, mask) for mask in range(nb - 1, 0, -1)]

    small = [
        pltpu.make_async_copy(idx_hbm, idx_ref, idx_sem.at[0]),
        pltpu.make_async_copy(tab_hbm, tab_ref, idx_sem.at[1]),
    ]
    for j in range(bases, -1, -1):
        table_copy(j).start()
    grid_copy(0).start()
    for copy in small:
        copy.start()

    barrier = pltpu.get_barrier_semaphore()
    for peer in others:
        pl.semaphore_signal(barrier, inc=1, device_id=(chan, peer), device_id_type=MESH)
    pl.semaphore_signal(barrier, inc=1, device_id=(mate, band), device_id_type=MESH)

    @pl.when(place < line - 1)
    def _():
        pl.semaphore_signal(barrier, inc=1, device_id=(chan + 2, band), device_id_type=MESH)

    def transform(t, begin, stop):
        def pair(i, carry):
            grid_flat = grid_v.reshape(2, tiles, outer * SUB, LANES)
            cols = []
            for k in range(2):
                r = i * 2 + k
                cols.append(
                    jnp.concatenate(
                        [grid_flat[p, t, pl.ds(r, outer, stride=SUB), :] for p in range(2)], axis=0
                    )
                )
            x = jnp.concatenate(cols, axis=1)
            high = x.astype(jnp.bfloat16)
            low = (x - high.astype(jnp.float32)).astype(jnp.bfloat16)
            mid = jnp.dot(
                first_v[...],
                jnp.concatenate([high, high, low], axis=0),
                preferred_element_type=jnp.float32,
            )
            turn_re, turn_im = turn_v[0], turn_v[1]
            turned = []
            for k in range(2):
                re = mid[:outer, k * LANES : (k + 1) * LANES]
                im = mid[outer:, k * LANES : (k + 1) * LANES]
                turned.append(
                    jnp.concatenate(
                        [re * turn_re - im * turn_im, re * turn_im + im * turn_re], axis=1
                    )
                )
            y = jnp.concatenate(turned, axis=0)
            high = y.astype(jnp.bfloat16)
            low = (y - high.astype(jnp.float32)).astype(jnp.bfloat16)
            out = lax.dot_general(
                second_v[...],
                jnp.concatenate([high, high, low], axis=1),
                (((1,), (1,)), ((), ())),
                preferred_element_type=jnp.float32,
            )
            flat = out_v.reshape(tiles, LANES * 2 * SUB, outer)
            for k in range(2):
                for p in range(2):
                    flat[t, pl.ds(p * SUB + i * 2 + k, LANES, stride=2 * SUB), :] = out[
                        p * LANES : (p + 1) * LANES, k * outer : (k + 1) * outer
                    ]
            return carry

        lax.fori_loop(begin // 2, stop // 2, pair, 0)

    def piece_send(j, peer):
        t, begin, size = pieces[j]
        return pltpu.make_async_remote_copy(
            src_ref=out_v.at[t, pl.ds(peer * kept * 2, kept * 2), pl.ds(begin, size), :],
            dst_ref=recv_v.at[band * tiles + t, :, pl.ds(begin, size), :],
            send_sem=bs_sem.at[0],
            recv_sem=er_sem.at[0],
            device_id=(chan, peer),
            device_id_type=MESH,
        )

    def slice_send(q, peer):
        return pltpu.make_async_remote_copy(
            src_ref=out_v.at[pl.ds(early, late), pl.ds((peer * kept + q * span) * 2, span * 2)],
            dst_ref=recv_v.at[pl.ds(band * tiles + early, late), pl.ds(q * span * 2, span * 2)],
            send_sem=bs_sem.at[0],
            recv_sem=lr_sem.at[q],
            device_id=(chan, peer),
            device_id_type=MESH,
        )

    def keep(t):
        recv_v[band * tiles + t] = out_v[t, pl.ds(band * kept * 2, kept * 2)]

    def flip(q):
        flip_slice(recv_v, spec_ref, q * span, span)

    coeffs = []

    def weigh(c):
        part, begin, size = cells[c]

        def one(j, carry):
            spot = (j % 2) * line + j // 2
            for q in range(begin // LANES, (begin + size) // LANES):
                sums = [None] * 3
                for ch in range(count):
                    x = res_v[ch, part, j, q]
                    for t in range(3):
                        term = coeffs[ch][t] * x
                        sums[t] = term if ch == 0 else sums[t] + term
                for t in range(3):
                    part_v[part, spot, pl.ds(t * SUB, SUB), pl.ds(q * LANES, LANES)] = sums[t]
            return carry

        lax.fori_loop(0, nc, one, 0)

    def landed(ref, sem):
        pltpu.make_async_copy(ref, ref, sem).wait()

    def pair_send(c):
        part, left, width = cells[c]
        at = pl.ds(left, width)
        return pltpu.make_async_remote_copy(
            src_ref=part_v.at[part, pl.ds((1 - core) * line, line), :, at],
            dst_ref=pair_v.at[part, :, :, at],
            send_sem=zs_sem.at[0],
            recv_sem=pair_sem.at[c],
            device_id=(mate, band),
            device_id_type=MESH,
        )

    def pair_add(c):
        part, left, width = cells[c]
        at = pl.ds(left, width)
        landed(pair_v.at[part, :, :, at], pair_sem.at[c])

        def one(k, carry):
            part_v[part, core * line + k, :, at] = part_v[part, core * line + k, :, at] + pair_v[part, k, :, at]
            return carry

        lax.fori_loop(0, line, one, 0)

    def facing(hop):
        return (place == line - 1 - hop).astype(jnp.int32)

    def line_send(p, hop, c):
        part, left, width = cells[c]
        at = pl.ds(left, width)
        down = facing(hop)
        spot = core * line + line - 1 - p + down * (2 * p - line + 1)
        last = hop + 1 == line - 1 - p
        sem = fin_sem.at[down * parts + part] if last else fw_sem.at[(down * (line - 2) + p) * chunks + c]
        return pltpu.make_async_remote_copy(
            src_ref=part_v.at[part, spot, :, at],
            dst_ref=land_v.at[down * (line - 1) + p, part, :, at],
            send_sem=zs_sem.at[0],
            recv_sem=sem,
            device_id=(chan + 2 - 4 * down, band),
            device_id_type=MESH,
        )

    def set_out(p, c):
        @pl.when((place == 0) | (place == line - 1))
        def _():
            line_send(p, 0, c).start()

    def forward(p, hop, c):
        @pl.when((place == hop) | (place == line - 1 - hop))
        def _():
            part, left, width = cells[c]
            at = pl.ds(left, width)
            down = facing(hop)
            spot = core * line + line - 1 - p + down * (2 * p - line + 1)
            row = down * (line - 1) + p
            landed(land_v.at[row, part, :, at], fw_sem.at[(down * (line - 2) + p) * chunks + c])
            part_v[part, spot, :, at] = part_v[part, spot, :, at] + land_v[row, part, :, at]
            line_send(p, hop, c).start()

    def finish(part):
        own = core * line + place

        @pl.when(place > 0)
        def _():
            row = line - 1 - place
            landed(land_v.at[row, part], fin_sem.at[part])
            part_v[part, own] = part_v[part, own] + land_v[row, part]

        @pl.when(place < line - 1)
        def _():
            row = line - 1 + place
            landed(land_v.at[row, part], fin_sem.at[parts + part])
            part_v[part, own] = part_v[part, own] + land_v[row, part]

        aa, ab, ac, bb, bc, cc = solved
        table = ((aa, ab, ac), (ab, bb, bc), (ac, bc, cc))
        for q in range(wide // LANES):
            at = pl.ds(q * LANES, LANES)
            tay = [part_v[part, own, pl.ds(t * SUB, SUB), at] for t in range(3)]
            for t, row in enumerate(table):
                comp_ref[t, pl.ds(part * SUB, SUB), at] = row[0] * tay[0] + row[1] * tay[1] + row[2] * tay[2]

    def mom_send(way):
        return pltpu.make_async_remote_copy(
            src_ref=mom_v.at[(0, 2, 3)[way]],
            dst_ref=mom_land.at[way],
            send_sem=ms_sem.at[way],
            recv_sem=mr_sem.at[way],
            device_id=((mate, chan + 2, chan - 2)[way], band),
            device_id_type=MESH,
        )

    def mom_pair():
        mom_send(0).wait_recv()
        mom_v[1] = mom_v[0] + mom_land[0]

        @pl.when(place < line - 1)
        def _():
            pl.semaphore_wait(ok_sem, 1)

        mom_hop(0)

    def mom_hop(hop):
        for way, from_end in ((1, place), (2, line - 1 - place)):

            @pl.when(from_end == hop)
            def _(way=way):
                if hop:
                    mom_send(way).wait_recv()
                    mom_v[way + 1] = mom_v[1] + mom_land[way]
                else:
                    mom_v[way + 1] = mom_v[1]
                if hop < line - 1:
                    mom_send(way).start()

    solved = []

    def mom_close():
        mom_hop(line - 1)
        mom_v[4] = mom_v[2]

        @pl.when(place < line - 1)
        def _():
            mom_v[4] = mom_v[2] + mom_land[2]

        for entry in inverse_rows(mom_v[4]):
            solved.append(jnp.broadcast_to(entry, (SUB, LANES)))

    weighed = added = 0

    def ready(c):
        for j, (first, _, begin, _) in enumerate(res_reads(parts, wide)):
            if cells[c][:2] == (first, begin):
                res_copy(j).wait()
        weigh(c)

    def spread(target):
        nonlocal weighed
        while weighed < min(target, chunks):
            ready(weighed)
            pair_send(weighed).start()
            weighed += 1

    def gather(target):
        nonlocal added
        while added < min(target, chunks):
            pair_add(added)
            for p, c in leaving:
                if added == c and (p == 0 or c < 2) or added == chunks - 1 > 1 and p > 0 and c >= 2:
                    set_out(p, c)
            added += 1

    for j in range(bases, -1, -1):
        table_copy(j).wait()
    grid_copy(0).wait()
    grids, reads = len(grid_reads(tiles)), len(res_reads(parts, wide))
    for j in range(max(grids - 1, reads)):
        if j < reads:
            res_copy(j).start()
        if j + 1 < grids:
            grid_copy(j + 1).start()

    for copy in small:
        copy.wait()
    total = count * nc
    moments = [jnp.float32(0.0)] * 5
    for c in range(count):
        weight = tab_ref[idx_ref[c]]
        position = (chan * count + c).astype(jnp.float32)
        offset = (2.0 * position + 1.0) * (1.0 / total) - 1.0
        power = weight
        trio = []
        for j in range(5):
            if j < 3:
                trio.append(power)
            moments[j] = moments[j] + power
            power = power * offset
        coeffs.append(trio)
    level = lax.broadcasted_iota(jnp.int32, (SUB, LANES), 0)
    tile = jnp.zeros((SUB, LANES), jnp.float32)
    for j in range(5):
        tile = jnp.where(level == j, moments[j], tile)
    mom_v[0] = tile

    def open_pieces():
        landed(recv_v.at[pl.ds(0, (nb - 1) * early)], er_sem.at[0])

    def flip_go(q):
        landed(recv_v.at[pl.ds(0, (nb - 1) * late), pl.ds(0, span * 2)], lr_sem.at[q])
        if q < slices - 1:
            flip(q)

    leaving = [(p, c) for c in range(min(2, chunks)) for p in range(line - 1)]
    leaving += [(p, c) for p in range(line - 1) for c in range(2, chunks)]
    jobs, clock = [], 9.0
    for p, c in leaving:
        takes = 12.6 * cells[c][2] / (parts * wide)
        clock += takes
        for hop in range(1, line - 1 - p):
            jobs.append((clock + (hop - 1) * (2.5 + takes), hop, forward, (p, hop, c)))
    for hop in range(1, line - 1):
        jobs.append((9.0 + 5.0 * hop, 0, mom_hop, (hop,)))
    jobs.append((30.0, 0, mom_close, ()))
    for part in range(parts):
        jobs.append((48.0 - 4.2 * (parts - 1 - part), 20, finish, (part,)))
    jobs.append((31.5, 9, open_pieces, ()))
    for q in range(slices):
        jobs.append((33.0 + 22.5 * (q + 1) / slices, 10, flip_go, (q,)))
    jobs.sort(key=lambda job: job[:2])

    half = SUB // 2
    ends = {(t, begin + size): j for j, (t, begin, size) in enumerate(pieces)}
    for unit in range(2 * tiles):
        t, begin = unit // 2, unit % 2 * half
        if unit == 2:
            for j in range(2, grids):
                grid_copy(j).wait()
        for top in range(begin, begin + half, HEAD if unit == 0 else half):
            stop = top + (HEAD if unit == 0 else half)
            if unit == 0 and top == HEAD:
                grid_copy(1).wait()
            transform(t, top, stop)
            if unit == 0 and top == 0:
                pl.semaphore_wait(barrier, nb + (place > 0).astype(jnp.int32))

                @pl.when(place > 0)
                def _():
                    pl.semaphore_signal(ok_sem, inc=1, device_id=(chan - 2, band), device_id_type=MESH)

            j = ends.get((t, stop))
            if j is not None:
                for peer in others:
                    piece_send(j, peer).start()
            if unit == 0 and top == 0:
                mom_send(0).start()
        if unit == 0:
            spread(2)
            mom_pair()
            gather(1)
        else:
            gather(unit + 1)
            spread(unit + 2)
        while jobs and jobs[0][0] < 7.5 + 2.05 * unit:
            _, _, work, args = jobs.pop(0)
            work(*args)
        if begin:
            keep(t)
    for q in range(slices):
        for peer in others:
            slice_send(q, peer).start()
    spread(chunks)
    gather(chunks)

    for _, _, work, args in jobs:
        work(*args)

    def drain_z():
        mom_send(0).wait_send()
        for way, sends in ((1, place < line - 1), (2, place > 0)):

            @pl.when(sends)
            def _(way=way):
                mom_send(way).wait_send()

        landed(part_v.at[:, pl.ds(0, nc - 1)], zs_sem.at[0])

    def drain_band():
        landed(recv_v.at[pl.ds(0, (nb - 1) * tiles)], bs_sem.at[0])

    drain_z()
    drain_band()


def crossed(index, size, mask):
    peer = 0
    for bit in range(int(math.log2(size))):
        own = (index // (1 << bit)) % 2
        peer = peer + (1 - own if mask >> bit & 1 else own) * (1 << bit)
    return peer


def flip_slice(recv_v, spec_ref, first, span):
    rows, outer = recv_v.shape[0] * SUB, recv_v.shape[3]

    def one(k, carry):
        for p in range(2):
            block = recv_v[:, (first + k) * 2 + p].reshape(rows, outer)
            spec_ref[p, 0, pl.ds(pl.multiple_of((first + k) * outer, LANES), outer), :] = block.T
        return carry

    lax.fori_loop(0, span, one, 0, unroll=2 if span % 2 == 0 else 1)


def chunk_list(parts, wide):
    first = wide // 4
    return [(0, 0, first), (0, first, wide - first)] + [(part, 0, wide) for part in range(1, parts)]


def head_pieces(tiles):
    early = tiles // 2
    half = SUB // 2
    first = [(0, top, HEAD) for top in range(0, half, HEAD)] + [(0, half, half)]
    return (first if early else []) + [(t, 0, SUB) for t in range(1, early)]


def grid_reads(tiles):
    reads = [(0, 1, 0, HEAD), (0, 1, HEAD, SUB - HEAD)]
    return reads + [(1, tiles - 1, 0, SUB)] * (tiles > 1)


def res_reads(parts, wide):
    first = wide // 4
    return [(0, 1, 0, first), (0, 1, first, wide - first), (1, parts - 1, 0, wide)]


def place_kernel(slices, spec_ref, comp_ref, recv_ref, spec_hbm, comp_hbm, spec_v, sem):
    rows = spec_ref.shape[2] // slices
    ready = rows * (slices - 1)
    span = recv_ref.shape[1] // 2 // slices
    copies = [
        pltpu.make_async_copy(spec_ref.at[p, 0, pl.ds(0, ready)], spec_hbm.at[p, 0, pl.ds(0, ready)], sem.at[p])
        for p in range(2)
    ]
    copies.append(pltpu.make_async_copy(comp_ref, comp_hbm, sem.at[2]))
    for copy in copies:
        copy.start()
    many, outer = recv_ref.shape[0] * SUB, recv_ref.shape[3]
    for k in range(span):
        for p in range(2):
            block = recv_ref[:, (span * (slices - 1) + k) * 2 + p].reshape(many, outer)
            spec_v[p, pl.ds(k * outer, outer), :] = block.T
    copies.append(pltpu.make_async_copy(spec_v, spec_hbm.at[:, 0, pl.ds(ready, rows)], sem.at[3]))
    copies[-1].start()
    for copy in copies:
        copy.wait()


def local(nc, nb, residual, weight_index, weight_table, gridded):
    count, row_count, columns = residual.shape
    _, groups, rows, length = gridded.shape
    outer = length // LANES
    tiles, parts = rows // SUB, row_count // SUB
    wide = columns // nc
    kept = LANES // nb
    slices = min(8, kept)
    line = nc // 2
    view = gridded.reshape(2, tiles, SUB, outer, LANES)
    view = jnp.transpose(view, (0, 1, 3, 2, 4))
    pixels = residual.reshape(count, parts, SUB, nc, wide // LANES, LANES)
    pixels = jnp.transpose(pixels, (0, 1, 3, 4, 2, 5))
    vmem = pl.BlockSpec(memory_space=pltpu.VMEM)
    hbm = pl.BlockSpec(memory_space=pl.ANY)
    dma = pltpu.SemaphoreType.DMA
    consts = [jnp.asarray(table) for table in tables(length)]
    bases = len(consts) - 1
    shape_spec = (2, 1, kept * outer, nb * rows)
    shape_comp = (3, row_count, wide)
    shape_recv = (nb * tiles, kept * 2, SUB, outer)
    chunks = len(chunk_list(parts, wide))
    held = pl.pallas_call(
        functools.partial(exchange_kernel, nc, nb, bases),
        out_shape=tuple(pltpu.VMEM(shape, jnp.float32) for shape in (shape_spec, shape_comp, shape_recv)),
        in_specs=[hbm] * (bases + 5),
        out_specs=(vmem, vmem, vmem),
        scratch_shapes=[
            *[pltpu.VMEM(c.shape, c.dtype) for c in consts],
            pltpu.SMEM(weight_index.shape, jnp.int32),
            pltpu.SMEM(weight_table.shape, jnp.float32),
            pltpu.VMEM((2, tiles, outer, SUB, LANES), jnp.float32),
            pltpu.VMEM((tiles, LANES * 2, SUB, outer), jnp.float32),
            pltpu.VMEM(pixels.shape, jnp.float32),
            pltpu.VMEM((parts, nc, 3 * SUB, wide), jnp.float32),
            pltpu.VMEM((parts, line, 3 * SUB, wide), jnp.float32),
            pltpu.VMEM((2 * (line - 1), parts, 3 * SUB, wide), jnp.float32),
            pltpu.VMEM((5, SUB, LANES), jnp.float32),
            pltpu.VMEM((3, SUB, LANES), jnp.float32),
            dma((2,)),
            dma((bases + 1,)),
            dma((len(grid_reads(tiles)),)),
            dma((len(res_reads(parts, wide)),)),
            dma((1,)),
            dma((1,)),
            dma((slices,)),
            dma((1,)),
            dma((chunks,)),
            dma((2 * (line - 2) * chunks,)),
            dma((2 * parts,)),
            dma((3,)),
            dma((3,)),
            pltpu.SemaphoreType.REGULAR,
        ],
        compiler_params=pltpu.CompilerParams(
            collective_id=0, has_side_effects=True, vmem_limit_bytes=58_000_000
        ),
        name="exchange",
    )(weight_index, weight_table, *consts, pixels, view)
    spectrum, components = pl.pallas_call(
        functools.partial(place_kernel, slices),
        out_shape=(
            jax.ShapeDtypeStruct(shape_spec, jnp.float32),
            jax.ShapeDtypeStruct(shape_comp, jnp.float32),
        ),
        in_specs=[vmem, vmem, vmem],
        out_specs=(hbm, hbm),
        scratch_shapes=[
            pltpu.VMEM((2, kept * outer // slices, nb * rows), jnp.float32),
            dma((4,)),
        ],
        compiler_params=pltpu.CompilerParams(vmem_limit_bytes=16 * 1024 * 1024),
        name="place",
    )(*held)
    return (components, spectrum)


def solution(mesh):
    nc, nb = mesh.shape["chan"], mesh.shape["band"]
    in_specs = (P("chan", "band", None), P("chan"), P(), P(None, "chan", "band", None))
    out_specs = (P(None, "band", "chan"), P(None, "chan", "band", None))
    return jax.shard_map(
        functools.partial(local, nc, nb),
        mesh=mesh,
        in_specs=in_specs,
        out_specs=out_specs,
        check_vma=False,
    )
```

```python
import functools
import math

import jax
import jax.numpy as jnp
import numpy as np
from jax import lax
from jax.experimental import pallas as pl
from jax.experimental.pallas import tpu as pltpu
from jax.sharding import PartitionSpec as P

MESH = pl.DeviceIdType.MESH
LANES = 128
SUB = 8
HEAD = 2


def block_form(table):
    real = np.block([[table.real, -table.imag], [table.imag, table.real]]).astype(np.float32)
    high = real.astype(jnp.bfloat16)
    low = (real - high.astype(np.float32)).astype(jnp.bfloat16)
    return np.concatenate([high, low, high], axis=1)


def dft(size):
    grid = np.outer(np.arange(size), np.arange(size)) % size
    return np.exp(-2j * np.pi * grid / size)


def tables(length):
    outer = length // LANES
    turn = np.exp(-2j * np.pi * np.outer(np.arange(outer), np.arange(LANES)) / length)
    turn = turn / math.sqrt(length)
    bases = [block_form(dft(outer))]
    if outer != LANES:
        bases.append(block_form(dft(LANES)))
    return (np.stack([turn.real, turn.imag]).astype(np.float32), *bases)


def inverse_rows(moment):
    s0, s1, s2, s3, s4 = (moment[j : j + 1, :] for j in range(5))
    aa = s2 * s4 - s3 * s3
    ab = s2 * s3 - s1 * s4
    ac = s1 * s3 - s2 * s2
    bb = s0 * s4 - s2 * s2
    bc = s1 * s2 - s0 * s3
    cc = s0 * s2 - s1 * s1
    determ = s0 * aa + s1 * ab + s2 * ac
    return [entry / determ for entry in (aa, ab, ac, bb, bc, cc)]


def exchange_kernel(nc, nb, bases, idx_hbm, tab_hbm, *rest):
    line = nc // 2
    tables_hbm, (res_hbm, grid_hbm) = rest[: bases + 1], rest[bases + 1 : bases + 3]
    spec_ref, comp_ref, recv_v = rest[bases + 3 : bases + 6]
    rest = rest[bases + 6 :]
    tables_v, rest = rest[: bases + 1], rest[bases + 1 :]
    (idx_ref, tab_ref, grid_v, out_v, res_v, part_v, pair_v, land_v, mom_v, mom_land) = rest[:10]
    (idx_sem, tab_sem, grid_sem, res_sem, bs_sem, er_sem, lr_sem) = rest[10:17]
    (zs_sem, pair_sem, fw_sem, fin_sem, ms_sem, mr_sem, ok_sem) = rest[17:]
    turn_v, first_v, second_v = tables_v[0], tables_v[1], tables_v[-1]
    chan = lax.axis_index("chan")
    band = lax.axis_index("band")
    tiles, outer = grid_v.shape[1], grid_v.shape[2]
    kept = LANES // nb
    count, parts = res_v.shape[0], res_v.shape[1]
    wide = part_v.shape[3]
    cells = chunk_list(parts, wide)
    chunks = len(cells)
    early = tiles // 2
    late = tiles - early
    pieces = head_pieces(tiles)
    slices = min(8, kept)
    span = kept // slices
    joined = slices - lr_sem.shape[0] + 1

    def table_copy(j):
        return pltpu.make_async_copy(tables_hbm[j], tables_v[j], tab_sem.at[j])

    def grid_copy(j):
        first, count, begin, size = grid_reads(tiles)[j]
        at = (slice(None), pl.ds(first, count), slice(None), pl.ds(begin, size))
        return pltpu.make_async_copy(grid_hbm.at[at], grid_v.at[at], grid_sem.at[j])

    def res_copy(j):
        first, many, begin, size = res_reads(parts, wide)[j]
        at = (slice(None), pl.ds(first, many), slice(None), pl.ds(begin // LANES, size // LANES))
        return pltpu.make_async_copy(res_hbm.at[at], res_v.at[at], res_sem.at[j])

    core, place = chan % 2, chan // 2
    mate = chan + 1 - 2 * core
    others = [crossed(band, nb, mask) for mask in range(nb - 1, 0, -1)]

    small = [
        pltpu.make_async_copy(idx_hbm, idx_ref, idx_sem.at[0]),
        pltpu.make_async_copy(tab_hbm, tab_ref, idx_sem.at[1]),
    ]
    for j in range(bases, -1, -1):
        table_copy(j).start()
    grid_copy(0).start()
    for copy in small:
        copy.start()

    barrier = pltpu.get_barrier_semaphore()
    for peer in others:
        pl.semaphore_signal(barrier, inc=1, device_id=(chan, peer), device_id_type=MESH)
    pl.semaphore_signal(barrier, inc=1, device_id=(mate, band), device_id_type=MESH)

    @pl.when(place < line - 1)
    def _():
        pl.semaphore_signal(barrier, inc=1, device_id=(chan + 2, band), device_id_type=MESH)

    def transform(t, begin, stop):
        def pair(i, carry):
            grid_flat = grid_v.reshape(2, tiles, outer * SUB, LANES)
            cols = []
            for k in range(2):
                r = i * 2 + k
                cols.append(
                    jnp.concatenate(
                        [grid_flat[p, t, pl.ds(r, outer, stride=SUB), :] for p in range(2)], axis=0
                    )
                )
            x = jnp.concatenate(cols, axis=1)
            high = x.astype(jnp.bfloat16)
            low = (x - high.astype(jnp.float32)).astype(jnp.bfloat16)
            mid = jnp.dot(
                first_v[...],
                jnp.concatenate([high, high, low], axis=0),
                preferred_element_type=jnp.float32,
            )
            turn_re, turn_im = turn_v[0], turn_v[1]
            turned = []
            for k in range(2):
                re = mid[:outer, k * LANES : (k + 1) * LANES]
                im = mid[outer:, k * LANES : (k + 1) * LANES]
                turned.append(
                    jnp.concatenate(
                        [re * turn_re - im * turn_im, re * turn_im + im * turn_re], axis=1
                    )
                )
            y = jnp.concatenate(turned, axis=0)
            high = y.astype(jnp.bfloat16)
            low = (y - high.astype(jnp.float32)).astype(jnp.bfloat16)
            out = lax.dot_general(
                second_v[...],
                jnp.concatenate([high, high, low], axis=1),
                (((1,), (1,)), ((), ())),
                preferred_element_type=jnp.float32,
            )
            flat = out_v.reshape(tiles, LANES * 2 * SUB, outer)
            for k in range(2):
                for p in range(2):
                    flat[t, pl.ds(p * SUB + i * 2 + k, LANES, stride=2 * SUB), :] = out[
                        p * LANES : (p + 1) * LANES, k * outer : (k + 1) * outer
                    ]
            return carry

        lax.fori_loop(begin // 2, stop // 2, pair, 0)

    def piece_send(j, peer):
        t, begin, size = pieces[j]
        return pltpu.make_async_remote_copy(
            src_ref=out_v.at[t, pl.ds(peer * kept * 2, kept * 2), pl.ds(begin, size), :],
            dst_ref=recv_v.at[band * tiles + t, :, pl.ds(begin, size), :],
            send_sem=bs_sem.at[0],
            recv_sem=er_sem.at[0],
            device_id=(chan, peer),
            device_id_type=MESH,
        )

    def slice_send(q, peer):
        return pltpu.make_async_remote_copy(
            src_ref=out_v.at[pl.ds(early, late), pl.ds((peer * kept + q * span) * 2, span * 2)],
            dst_ref=recv_v.at[pl.ds(band * tiles + early, late), pl.ds(q * span * 2, span * 2)],
            send_sem=bs_sem.at[0],
            recv_sem=lr_sem.at[max(q - joined + 1, 0)],
            device_id=(chan, peer),
            device_id_type=MESH,
        )

    def keep(t):
        recv_v[band * tiles + t] = out_v[t, pl.ds(band * kept * 2, kept * 2)]

    def flip(q):
        flip_slice(recv_v, spec_ref, q * span, span)

    coeffs = []

    def weigh(c):
        part, begin, size = cells[c]

        def one(j, carry):
            spot = (j % 2) * line + j // 2
            for q in range(begin // LANES, (begin + size) // LANES):
                sums = [None] * 3
                for ch in range(count):
                    x = res_v[ch, part, j, q]
                    for t in range(3):
                        term = coeffs[ch][t] * x
                        sums[t] = term if ch == 0 else sums[t] + term
                for t in range(3):
                    part_v[part, spot, pl.ds(t * SUB, SUB), pl.ds(q * LANES, LANES)] = sums[t]
            return carry

        lax.fori_loop(0, nc, one, 0)

    def landed(ref, sem):
        pltpu.make_async_copy(ref, ref, sem).wait()

    def pair_send(c):
        part, left, width = cells[c]
        at = pl.ds(left, width)
        return pltpu.make_async_remote_copy(
            src_ref=part_v.at[part, pl.ds((1 - core) * line, line), :, at],
            dst_ref=pair_v.at[part, :, :, at],
            send_sem=zs_sem.at[0],
            recv_sem=pair_sem.at[c],
            device_id=(mate, band),
            device_id_type=MESH,
        )

    def pair_add(c):
        part, left, width = cells[c]
        at = pl.ds(left, width)
        landed(pair_v.at[part, :, :, at], pair_sem.at[c])

        def one(k, carry):
            part_v[part, core * line + k, :, at] = part_v[part, core * line + k, :, at] + pair_v[part, k, :, at]
            return carry

        lax.fori_loop(0, line, one, 0)

    def facing(hop):
        return (place == line - 1 - hop).astype(jnp.int32)

    def line_send(p, hop, c):
        part, left, width = cells[c]
        at = pl.ds(left, width)
        down = facing(hop)
        spot = core * line + line - 1 - p + down * (2 * p - line + 1)
        last = hop + 1 == line - 1 - p
        sem = fin_sem.at[down * parts + part] if last else fw_sem.at[(down * (line - 2) + p) * parts + part]
        return pltpu.make_async_remote_copy(
            src_ref=part_v.at[part, spot, :, at],
            dst_ref=land_v.at[down * (line - 1) + p, part, :, at],
            send_sem=zs_sem.at[0],
            recv_sem=sem,
            device_id=(chan + 2 - 4 * down, band),
            device_id_type=MESH,
        )

    def set_out(p, c):
        @pl.when((place == 0) | (place == line - 1))
        def _():
            line_send(p, 0, c).start()

    def forward(p, hop, c):
        @pl.when((place == hop) | (place == line - 1 - hop))
        def _():
            part = cells[c][0]
            down = facing(hop)
            spot = core * line + line - 1 - p + down * (2 * p - line + 1)
            row = down * (line - 1) + p
            landed(land_v.at[row, part], fw_sem.at[(down * (line - 2) + p) * parts + part])
            part_v[part, spot] = part_v[part, spot] + land_v[row, part]
            for k, cell in enumerate(cells):
                if cell[0] == part:
                    line_send(p, hop, k).start()

    def finish(part):
        own = core * line + place

        @pl.when(place > 0)
        def _():
            row = line - 1 - place
            landed(land_v.at[row, part], fin_sem.at[part])
            part_v[part, own] = part_v[part, own] + land_v[row, part]

        @pl.when(place < line - 1)
        def _():
            row = line - 1 + place
            landed(land_v.at[row, part], fin_sem.at[parts + part])
            part_v[part, own] = part_v[part, own] + land_v[row, part]

        aa, ab, ac, bb, bc, cc = solved
        table = ((aa, ab, ac), (ab, bb, bc), (ac, bc, cc))
        for q in range(wide // LANES):
            at = pl.ds(q * LANES, LANES)
            tay = [part_v[part, own, pl.ds(t * SUB, SUB), at] for t in range(3)]
            for t, row in enumerate(table):
                comp_ref[t, pl.ds(part * SUB, SUB), at] = row[0] * tay[0] + row[1] * tay[1] + row[2] * tay[2]

    def mom_send(way):
        return pltpu.make_async_remote_copy(
            src_ref=mom_v.at[(0, 2, 3)[way]],
            dst_ref=mom_land.at[way],
            send_sem=ms_sem.at[way],
            recv_sem=mr_sem.at[way],
            device_id=((mate, chan + 2, chan - 2)[way], band),
            device_id_type=MESH,
        )

    def mom_pair():
        mom_send(0).wait_recv()
        mom_v[1] = mom_v[0] + mom_land[0]

        @pl.when(place < line - 1)
        def _():
            pl.semaphore_wait(ok_sem, 1)

        mom_hop(0)

    def mom_hop(hop):
        for way, from_end in ((1, place), (2, line - 1 - place)):

            @pl.when(from_end == hop)
            def _(way=way):
                if hop:
                    mom_send(way).wait_recv()
                    mom_v[way + 1] = mom_v[1] + mom_land[way]
                else:
                    mom_v[way + 1] = mom_v[1]
                if hop < line - 1:
                    mom_send(way).start()

    solved = []

    def mom_close():
        mom_hop(line - 1)
        mom_v[4] = mom_v[2]

        @pl.when(place < line - 1)
        def _():
            mom_v[4] = mom_v[2] + mom_land[2]

        for entry in inverse_rows(mom_v[4]):
            solved.append(jnp.broadcast_to(entry, (SUB, LANES)))

    weighed = added = 0

    def ready(c):
        for j, (first, _, begin, _) in enumerate(res_reads(parts, wide)):
            if cells[c][:2] == (first, begin):
                res_copy(j).wait()
        weigh(c)

    def spread(target):
        nonlocal weighed
        while weighed < min(target, chunks):
            ready(weighed)
            pair_send(weighed).start()
            weighed += 1

    def gather(target):
        nonlocal added
        while added < min(target, chunks):
            pair_add(added)
            for p, c in leaving:
                if added == c and (p == 0 or c < 2) or added == chunks - 1 > 1 and p > 0 and c >= 2:
                    set_out(p, c)
            added += 1

    for j in range(bases, -1, -1):
        table_copy(j).wait()
    grid_copy(0).wait()
    grids, reads = len(grid_reads(tiles)), len(res_reads(parts, wide))
    for j in range(max(grids - 1, reads)):
        if j < reads:
            res_copy(j).start()
        if j + 1 < grids:
            grid_copy(j + 1).start()

    for copy in small:
        copy.wait()
    total = count * nc
    moments = [jnp.float32(0.0)] * 5
    for c in range(count):
        weight = tab_ref[idx_ref[c]]
        position = (chan * count + c).astype(jnp.float32)
        offset = (2.0 * position + 1.0) * (1.0 / total) - 1.0
        power = weight
        trio = []
        for j in range(5):
            if j < 3:
                trio.append(power)
            moments[j] = moments[j] + power
            power = power * offset
        coeffs.append(trio)
    level = lax.broadcasted_iota(jnp.int32, (SUB, LANES), 0)
    tile = jnp.zeros((SUB, LANES), jnp.float32)
    for j in range(5):
        tile = jnp.where(level == j, moments[j], tile)
    mom_v[0] = tile

    def open_pieces():
        landed(recv_v.at[pl.ds(0, (nb - 1) * early)], er_sem.at[0])

    def flip_go(q):
        if q < joined - 1:
            return
        first = 0 if q == joined - 1 else q
        many = q + 1 - first
        landed(recv_v.at[pl.ds(0, (nb - 1) * late), pl.ds(0, many * span * 2)], lr_sem.at[max(q - joined + 1, 0)])
        for k in range(first, min(q + 1, slices - 1)):
            flip(k)

    leaving = [(p, c) for c in range(min(2, chunks)) for p in range(line - 1)]
    leaving += [(p, c) for p in range(line - 1) for c in range(2, chunks)]
    jobs, clock = [], 9.0
    for p, c in leaving:
        takes = 12.6 * cells[c][2] / (parts * wide)
        clock += takes
        for hop in range(1, line - 1 - p if c else 1):
            jobs.append((clock + (hop - 1) * (2.5 + takes), hop, forward, (p, hop, c)))
    for hop in range(1, line - 1):
        jobs.append((9.0 + 5.0 * hop, 0, mom_hop, (hop,)))
    jobs.append((30.0, 0, mom_close, ()))
    for part in range(parts):
        jobs.append((48.0 - 4.2 * (parts - 1 - part), 20, finish, (part,)))
    jobs.append((31.5, 9, open_pieces, ()))
    for q in range(slices):
        jobs.append((33.0 + 22.5 * (q + 1) / slices, 10, flip_go, (q,)))
    jobs.sort(key=lambda job: job[:2])

    half = SUB // 2
    ends = {(t, begin + size): j for j, (t, begin, size) in enumerate(pieces)}
    for unit in range(2 * tiles):
        t, begin = unit // 2, unit % 2 * half
        if unit == 2:
            for j in range(2, grids):
                grid_copy(j).wait()
        for top in range(begin, begin + half, HEAD if unit == 0 else half):
            stop = top + (HEAD if unit == 0 else half)
            if unit == 0 and top == HEAD:
                grid_copy(1).wait()
            transform(t, top, stop)
            if unit == 0 and top == 0:
                pl.semaphore_wait(barrier, nb + (place > 0).astype(jnp.int32))

                @pl.when(place > 0)
                def _():
                    pl.semaphore_signal(ok_sem, inc=1, device_id=(chan - 2, band), device_id_type=MESH)

            j = ends.get((t, stop))
            if j is not None:
                for peer in others:
                    piece_send(j, peer).start()
            if unit == 0 and top == 0:
                mom_send(0).start()
        if unit == 0:
            spread(2)
            mom_pair()
            gather(1)
        else:
            gather(unit + 1)
            spread(unit + 2)
        while jobs and jobs[0][0] < 7.5 + 2.05 * unit:
            _, _, work, args = jobs.pop(0)
            work(*args)
        if begin:
            keep(t)
    for q in range(slices):
        for peer in others:
            slice_send(q, peer).start()
    spread(chunks)
    gather(chunks)

    for _, _, work, args in jobs:
        work(*args)

    def drain_z():
        mom_send(0).wait_send()
        for way, sends in ((1, place < line - 1), (2, place > 0)):

            @pl.when(sends)
            def _(way=way):
                mom_send(way).wait_send()

        landed(part_v.at[:, pl.ds(0, nc - 1)], zs_sem.at[0])

    def drain_band():
        landed(recv_v.at[pl.ds(0, (nb - 1) * tiles)], bs_sem.at[0])

    drain_z()
    drain_band()


def crossed(index, size, mask):
    peer = 0
    for bit in range(int(math.log2(size))):
        own = (index // (1 << bit)) % 2
        peer = peer + (1 - own if mask >> bit & 1 else own) * (1 << bit)
    return peer


def flip_slice(recv_v, spec_ref, first, span):
    rows, outer = recv_v.shape[0] * SUB, recv_v.shape[3]

    def one(k, carry):
        for p in range(2):
            block = recv_v[:, (first + k) * 2 + p].reshape(rows, outer)
            spec_ref[p, 0, pl.ds(pl.multiple_of((first + k) * outer, LANES), outer), :] = block.T
        return carry

    lax.fori_loop(0, span, one, 0, unroll=2 if span % 2 == 0 else 1)


def chunk_list(parts, wide):
    first = wide // 4
    return [(0, 0, first), (0, first, wide - first)] + [(part, 0, wide) for part in range(1, parts)]


def head_pieces(tiles):
    early = tiles // 2
    half = SUB // 2
    first = [(0, top, HEAD) for top in range(0, half, HEAD)] + [(0, half, half)]
    return (first if early else []) + [(t, 0, SUB) for t in range(1, early)]


def grid_reads(tiles):
    reads = [(0, 1, 0, HEAD), (0, 1, HEAD, SUB - HEAD)]
    return reads + [(1, tiles - 1, 0, SUB)] * (tiles > 1)


def res_reads(parts, wide):
    first = wide // 4
    return [(0, 1, 0, first), (0, 1, first, wide - first), (1, parts - 1, 0, wide)]


def place_kernel(slices, spec_ref, comp_ref, recv_ref, spec_hbm, comp_hbm, spec_v, sem):
    rows = spec_ref.shape[2] // slices
    ready = rows * (slices - 1)
    span = recv_ref.shape[1] // 2 // slices
    copies = [
        pltpu.make_async_copy(spec_ref.at[p, 0, pl.ds(0, ready)], spec_hbm.at[p, 0, pl.ds(0, ready)], sem.at[p])
        for p in range(2)
    ]
    copies.append(pltpu.make_async_copy(comp_ref, comp_hbm, sem.at[2]))
    for copy in copies:
        copy.start()
    many, outer = recv_ref.shape[0] * SUB, recv_ref.shape[3]
    for k in range(span):
        for p in range(2):
            block = recv_ref[:, (span * (slices - 1) + k) * 2 + p].reshape(many, outer)
            spec_v[p, pl.ds(k * outer, outer), :] = block.T
    copies.append(pltpu.make_async_copy(spec_v, spec_hbm.at[:, 0, pl.ds(ready, rows)], sem.at[3]))
    copies[-1].start()
    for copy in copies:
        copy.wait()


def local(nc, nb, residual, weight_index, weight_table, gridded):
    count, row_count, columns = residual.shape
    _, groups, rows, length = gridded.shape
    outer = length // LANES
    tiles, parts = rows // SUB, row_count // SUB
    wide = columns // nc
    kept = LANES // nb
    slices = min(8, kept)
    line = nc // 2
    view = gridded.reshape(2, tiles, SUB, outer, LANES)
    view = jnp.transpose(view, (0, 1, 3, 2, 4))
    pixels = residual.reshape(count, parts, SUB, nc, wide // LANES, LANES)
    pixels = jnp.transpose(pixels, (0, 1, 3, 4, 2, 5))
    vmem = pl.BlockSpec(memory_space=pltpu.VMEM)
    hbm = pl.BlockSpec(memory_space=pl.ANY)
    dma = pltpu.SemaphoreType.DMA
    consts = [jnp.asarray(table) for table in tables(length)]
    bases = len(consts) - 1
    shape_spec = (2, 1, kept * outer, nb * rows)
    shape_comp = (3, row_count, wide)
    shape_recv = (nb * tiles, kept * 2, SUB, outer)
    chunks = len(chunk_list(parts, wide))
    held = pl.pallas_call(
        functools.partial(exchange_kernel, nc, nb, bases),
        out_shape=tuple(pltpu.VMEM(shape, jnp.float32) for shape in (shape_spec, shape_comp, shape_recv)),
        in_specs=[hbm] * (bases + 5),
        out_specs=(vmem, vmem, vmem),
        scratch_shapes=[
            *[pltpu.VMEM(c.shape, c.dtype) for c in consts],
            pltpu.SMEM(weight_index.shape, jnp.int32),
            pltpu.SMEM(weight_table.shape, jnp.float32),
            pltpu.VMEM((2, tiles, outer, SUB, LANES), jnp.float32),
            pltpu.VMEM((tiles, LANES * 2, SUB, outer), jnp.float32),
            pltpu.VMEM(pixels.shape, jnp.float32),
            pltpu.VMEM((parts, nc, 3 * SUB, wide), jnp.float32),
            pltpu.VMEM((parts, line, 3 * SUB, wide), jnp.float32),
            pltpu.VMEM((2 * (line - 1), parts, 3 * SUB, wide), jnp.float32),
            pltpu.VMEM((5, SUB, LANES), jnp.float32),
            pltpu.VMEM((3, SUB, LANES), jnp.float32),
            dma((2,)),
            dma((bases + 1,)),
            dma((len(grid_reads(tiles)),)),
            dma((len(res_reads(parts, wide)),)),
            dma((1,)),
            dma((1,)),
            dma((slices - slices // 2 + 1,)),
            dma((1,)),
            dma((chunks,)),
            dma((2 * (line - 2) * parts,)),
            dma((2 * parts,)),
            dma((3,)),
            dma((3,)),
            pltpu.SemaphoreType.REGULAR,
        ],
        compiler_params=pltpu.CompilerParams(
            collective_id=0, has_side_effects=True, vmem_limit_bytes=58_000_000
        ),
        name="exchange",
    )(weight_index, weight_table, *consts, pixels, view)
    spectrum, components = pl.pallas_call(
        functools.partial(place_kernel, slices),
        out_shape=(
            jax.ShapeDtypeStruct(shape_spec, jnp.float32),
            jax.ShapeDtypeStruct(shape_comp, jnp.float32),
        ),
        in_specs=[vmem, vmem, vmem],
        out_specs=(hbm, hbm),
        scratch_shapes=[
            pltpu.VMEM((2, kept * outer // slices, nb * rows), jnp.float32),
            dma((4,)),
        ],
        compiler_params=pltpu.CompilerParams(vmem_limit_bytes=16 * 1024 * 1024),
        name="place",
    )(*held)
    return (components, spectrum)


def solution(mesh):
    nc, nb = mesh.shape["chan"], mesh.shape["band"]
    in_specs = (P("chan", "band", None), P("chan"), P(), P(None, "chan", "band", None))
    out_specs = (P(None, "band", "chan"), P(None, "chan", "band", None))
    return jax.shard_map(
        functools.partial(local, nc, nb),
        mesh=mesh,
        in_specs=in_specs,
        out_specs=out_specs,
        check_vma=False,
    )
```
